32 devices in a mesh: member: 2 (over y), gy: 4 (over z), gx: 2 (over x), lev: 2 (over core).
Axes of the slice: x: 2, y: 2, z: 4, core: 2. Of those that a mesh axis runs over, the one named last changes fastest.
Arguments:
- level_field: bfloat16 [32, 1536, 1536], P(('member', 'lev'), 'gy', 'gx'), parts along dimension 0, may hold values from -6 to 6
Outputs:
- spectra: float32 [1536, 32, 1536], P(('gy', 'gx'), ('member', 'lev')), parts along dimension 1
- spectra_zone: float32 [1536, 32, 11], P(('gy', 'gx'), ('member', 'lev')), parts along dimension 1
The draws below stay inside these ranges and needn't reach their ends.
There are 2 independent parts, one for each index of `member`. The reference program is written for one: setup_inputs(seed, part) draws one part's arguments, and reference() takes and returns one part's arrays. A program takes and returns all parts, laid end to end along the dimension named above; each array names one. Nothing has to cross between parts.
All inputs are finite; a program needn't handle non-finite values.
Results may differ from the reference program's by a relative error of at most 0.0042.
Values may be sent and summed in bfloat16 or wider, within the bound.
A program may use at most 128 MiB of HBM per device.

```python
import math
import jax
import jax.numpy as jnp
from jax import lax

NX = 1536
NY = 1536
EXT_ZONE = 11
WAVES = 768
LEVELS = 16


def shard_levels(own_key, shape, cuts, low, largest):
    gain, own = 1.0, jax.random.fold_in(own_key, 6)
    for axis_at, parts in cuts:
        draws = jnp.exp(jax.random.uniform(jax.random.fold_in(own, axis_at), (parts,), jnp.float32, low / len(cuts), largest / len(cuts)))
        gain = gain * jnp.repeat(draws, shape[axis_at] // parts).reshape([-1 if axis == axis_at else 1 for axis in range(len(shape))])
    return gain


def centred(stream_key, dims, deviation, most, split=(), kind=jnp.bfloat16):
    drawn = deviation * jax.random.normal(stream_key, dims, jnp.float32)
    if split:
        drawn = drawn * shard_levels(stream_key, dims, split, -0.22, 0.18)
    return jnp.clip(drawn, -most, most).astype(kind)


def setup_inputs(seed: int = 0, part: int = 0) -> dict:
    keys = jax.random.split(jax.random.key(seed), 2)
    part_splits = jax.random.split(jax.random.fold_in(keys[1], part), 2)
    return {
        "level_field": centred(part_splits[0], (LEVELS, NY, NX), 1.0, 6.0, ((0, 2), (1, 4), (2, 2))),
    }


def blend_zone(second_last, last_value, first_value, second_value, zone_count):
    steps = (jnp.arange(zone_count, dtype=jnp.int32) + 1).astype(jnp.float32) / (zone_count + 1.0)
    weight_a = 2.0 * steps ** 3 - 3.0 * steps ** 2 + 1.0
    weight_b = steps ** 3 - 2.0 * steps ** 2 + steps
    weight_c = -2.0 * steps ** 3 + 3.0 * steps ** 2
    weight_d = steps ** 3 - steps ** 2
    tangent_scale = zone_count + 1.0
    slope_start = tangent_scale * (last_value - second_last)
    slope_end = tangent_scale * (second_value - first_value)
    return last_value[..., None] * weight_a + slope_start[..., None] * weight_b + first_value[..., None] * weight_c + slope_end[..., None] * weight_d

def make_table(wave_count, length):
    coeff = jnp.arange(2 * wave_count, dtype=jnp.int32)[:, None]
    column = jnp.arange(length, dtype=jnp.int32)[None, :]
    is_cosine = coeff < wave_count
    number = jnp.where(is_cosine, coeff, coeff - wave_count + 1)
    phase = (number * column % length).astype(jnp.float32) * (2.0 * math.pi / length)
    values = jnp.where(is_cosine, jnp.cos(phase), -jnp.sin(phase)) / math.sqrt(length)
    return values.astype(jnp.bfloat16)

def reference(level_field):
    widened = level_field.astype(jnp.float32)
    zone_x = blend_zone(widened[..., NX - 2], widened[..., NX - 1], widened[..., 0], widened[..., 1], EXT_ZONE).astype(jnp.bfloat16)
    extended = jnp.concatenate([level_field, zone_x], axis=2)
    wave_table = make_table(WAVES, NX + EXT_ZONE)

    def one_level(level_rows):
        return lax.dot_general(wave_table, level_rows, (((1,), (1,)), ((), ())), preferred_element_type=jnp.float32)
    stacked = lax.map(one_level, extended)
    spectra = jnp.transpose(stacked, (1, 0, 2))
    spectra_zone = blend_zone(spectra[..., NY - 2], spectra[..., NY - 1], spectra[..., 0], spectra[..., 1], EXT_ZONE)
    return (spectra, spectra_zone)
```

```python
import functools
import math

import jax
import jax.numpy as jnp
import numpy as np
from jax import lax
from jax.experimental import pallas as pl
from jax.experimental.pallas import tpu as pltpu
from jax.sharding import PartitionSpec as P

EXT_ZONE = 11
LANES = 128
NT = (((1,), (1,)), ((), ()))
MESH = pl.DeviceIdType.MESH


def blend_weights(zone_count):
    steps = (jnp.arange(zone_count, dtype=jnp.int32) + 1).astype(jnp.float32) / (zone_count + 1.0)
    weight_a = 2.0 * steps**3 - 3.0 * steps**2 + 1.0
    weight_b = steps**3 - 2.0 * steps**2 + steps
    weight_c = -2.0 * steps**3 + 3.0 * steps**2
    weight_d = steps**3 - steps**2
    return weight_a, weight_b, weight_c, weight_d


def blend_zone(second_last, last_value, first_value, second_value, zone_count):
    weight_a, weight_b, weight_c, weight_d = blend_weights(zone_count)
    tangent_scale = zone_count + 1.0
    slope_start = tangent_scale * (last_value - second_last)
    slope_end = tangent_scale * (second_value - first_value)
    return (
        last_value[..., None] * weight_a
        + slope_start[..., None] * weight_b
        + first_value[..., None] * weight_c
        + slope_end[..., None] * weight_d
    )


def wave_factors(coeff0, group, column, wave_count, length):
    number0 = jnp.where(coeff0 < wave_count, coeff0, coeff0 - wave_count + 1)
    scale = 2.0 * math.pi / length
    phase0 = (number0[:, None] * column[None, :] % length).astype(jnp.float32) * scale
    cos0, sin0 = jnp.cos(phase0), jnp.sin(phase0)
    is_cosine = (coeff0 < wave_count)[:, None]
    p, q = jnp.where(is_cosine, cos0, -sin0), jnp.where(is_cosine, sin0, cos0)
    step = jnp.arange(group, dtype=jnp.int32)
    phase = (step[:, None] * column[None, :] % length).astype(jnp.float32) * scale
    norm = 1.0 / math.sqrt(length)
    return p, q, jnp.cos(phase) * norm, jnp.sin(phase) * norm


def kernel(n_gx, n_gy, field_ref, edge_ref, table_ref, ztable_ref, weight_ref,
           out_ref, out_edge_ref, xgot, xedge, send, esend, xs, xr, es, er, zs, zr, ts, tr):
    levels, rows, cols = field_ref.shape
    bands = table_ref.shape[2]
    me_x, me_y = lax.axis_index("gx"), lax.axis_index("gy")

    def peer_x(shift):
        return {"gx": lax.rem(me_x + n_gx - shift, n_gx)}

    def peer_y(shift):
        return {"gy": lax.rem(me_y + shift, n_gy)}

    barrier = pltpu.get_barrier_semaphore()
    for shift in range(1, n_gx):
        pl.semaphore_signal(barrier, inc=1, device_id=peer_x(shift), device_id_type=MESH)
    for shift in range(1, n_gy):
        pl.semaphore_signal(barrier, inc=1, device_id=peer_y(shift), device_id_type=MESH)
    pl.semaphore_wait(barrier, n_gx + n_gy - 2)

    def edge_x(shift):
        return pltpu.make_async_remote_copy(
            src_ref=edge_ref, dst_ref=xedge.at[shift - 1], send_sem=es.at[shift - 1],
            recv_sem=er.at[shift - 1], device_id=peer_x(shift), device_id_type=MESH)

    def rows_x(shift, level):
        return pltpu.make_async_remote_copy(
            src_ref=field_ref.at[level], dst_ref=xgot.at[shift - 1, level],
            send_sem=xs.at[shift - 1, level], recv_sem=xr.at[shift - 1, level],
            device_id=peer_x(shift), device_id_type=MESH)

    def edge_y(shift):
        return pltpu.make_async_remote_copy(
            src_ref=esend.at[shift - 1], dst_ref=out_edge_ref.at[shift], send_sem=ts.at[shift - 1],
            recv_sem=tr.at[shift - 1], device_id=peer_y(shift), device_id_type=MESH)

    def spec_y(shift, level):
        return pltpu.make_async_remote_copy(
            src_ref=send.at[shift - 1, level], dst_ref=out_ref.at[shift, level],
            send_sem=zs.at[shift - 1, level], recv_sem=zr.at[shift - 1, level],
            device_id=peer_y(shift), device_id_type=MESH)

    for shift in range(1, n_gx):
        edge_x(shift).start()

    @pl.loop(0, levels)
    def _(level):
        for shift in range(1, n_gx):
            rows_x(shift, level).start()

    tail = (cols - 1) // LANES * LANES

    def zone_of(parts):
        first = second = last = before = 0.0
        for at, part in enumerate(parts):
            owner = lax.rem(me_x + at, n_gx)
            is_first = jnp.where(owner == 0, 1.0, 0.0)
            is_last = jnp.where(owner == n_gx - 1, 1.0, 0.0)
            head = part[:, :min(LANES, cols)].astype(jnp.float32)
            rear = part[:, tail:].astype(jnp.float32)
            first += is_first * head[:, 0:1]
            second += is_first * head[:, 1:2]
            before += is_last * rear[:, cols - 2 - tail:cols - 1 - tail]
            last += is_last * rear[:, cols - 1 - tail:cols - tail]
        tangent = EXT_ZONE + 1.0
        zone = (last * weight_ref[0:1, :] + (tangent * (last - before)) * weight_ref[1:2, :]
                + first * weight_ref[2:3, :] + (tangent * (second - first)) * weight_ref[3:4, :])
        return zone.astype(jnp.bfloat16)

    def dot(a, b):
        return lax.dot_general(a, b, NT, preferred_element_type=jnp.float32)

    for shift in range(1, n_gx):
        edge_x(shift).wait_recv()
    parts = [edge_ref[...]] + [xedge[at] for at in range(n_gx - 1)]
    zone = zone_of(parts)
    for shift in range(n_gy):
        total = dot(zone, ztable_ref[shift])
        for at, part in enumerate(parts):
            total += dot(part, table_ref[at, shift])
        if shift == 0:
            out_edge_ref[0] = total
        else:
            esend[shift - 1] = total
            edge_y(shift).start()

    merged = bands % 16 == 0

    @pl.loop(0, levels)
    def _(level):
        for shift in range(1, n_gx):
            rows_x(shift, level).wait_recv()
        parts = [field_ref[level]] + [xgot[at, level] for at in range(n_gx - 1)]
        zone = zone_of(parts)
        if merged:
            size = n_gy * bands
            total = dot(ztable_ref[...].reshape(size, LANES), zone)
            for at, part in enumerate(parts):
                total += dot(table_ref[at].reshape(size, cols), part)
            pieces = [total[s * bands:(s + 1) * bands] for s in range(n_gy)]
        else:
            pieces = []
            for shift in range(n_gy):
                total = dot(ztable_ref[shift], zone)
                for at, part in enumerate(parts):
                    total += dot(table_ref[at, shift], part)
                pieces.append(total)
        for shift in range(n_gy):
            piece = pieces[shift].astype(jnp.bfloat16)
            if shift == 0:
                out_ref[0, level] = piece
            else:
                send[shift - 1, level] = piece
        for shift in range(1, n_gy):
            spec_y(shift, level).start()

    for shift in range(1, n_gx):
        edge_x(shift).wait_send()
    for shift in range(1, n_gy):
        edge_y(shift).wait()

    @pl.loop(0, levels)
    def _(level):
        for shift in range(1, n_gx):
            rows_x(shift, level).wait_send()
        for shift in range(1, n_gy):
            spec_y(shift, level).wait()


def make_plain_body(mesh):
    n_gx, n_gy = mesh.shape["gx"], mesh.shape["gy"]

    def body(field):
        levels, rows, cols = field.shape
        nx, ny = cols * n_gx, rows * n_gy
        length = nx + EXT_ZONE
        me_x, me_y = lax.axis_index("gx"), lax.axis_index("gy")
        bands = nx // (n_gx * n_gy)
        assert (nx // 2) % bands == 0
        group = 16 if bands % 16 == 0 else bands

        at = jnp.arange(nx + LANES, dtype=jnp.int32)
        column = jnp.where(at < nx, (at + me_x * cols) % nx, at)
        shift_at = jnp.arange(n_gy, dtype=jnp.int32)[:, None]
        coeff = ((me_y + shift_at) % n_gy) * (n_gx * bands) + me_x * bands
        coeff = (coeff + jnp.arange(0, bands, group, dtype=jnp.int32)[None, :]).reshape(-1)
        factors = wave_factors(coeff, group, column, nx // 2, length)
        p, q, c, s = lax.optimization_barrier(factors)

        def expand(lo, hi):
            full = p[:, None, lo:hi] * c[None, :, lo:hi] - q[:, None, lo:hi] * s[None, :, lo:hi]
            return full.astype(jnp.bfloat16).reshape(n_gy, bands, hi - lo)

        table = jnp.stack([expand(i * cols, (i + 1) * cols) for i in range(n_gx)])
        ztable = expand(nx, nx + LANES)
        ztable = jnp.where(jnp.arange(LANES) < EXT_ZONE, ztable, jnp.zeros_like(ztable))
        weights = jnp.pad(jnp.stack(blend_weights(EXT_ZONE)), ((0, 4), (0, LANES - EXT_ZONE)))
        edge = jnp.concatenate([field[:, :2], field[:, rows - 2:]], axis=1)
        edge = edge.transpose(1, 0, 2).reshape(4 * levels, cols)

        vmem = pl.BlockSpec(memory_space=pltpu.VMEM)
        dma = pltpu.SemaphoreType.DMA
        xs, ys = n_gx - 1, n_gy - 1
        got, edge_got = pl.pallas_call(
            functools.partial(kernel, n_gx, n_gy),
            out_shape=(
                jax.ShapeDtypeStruct((n_gy, levels, bands, rows), jnp.bfloat16),
                jax.ShapeDtypeStruct((n_gy, 4 * levels, bands), jnp.float32),
            ),
            in_specs=[vmem] * 5,
            out_specs=(vmem, vmem),
            scratch_shapes=[
                pltpu.VMEM((xs, levels, rows, cols), jnp.bfloat16),
                pltpu.VMEM((xs, 4 * levels, cols), jnp.bfloat16),
                pltpu.VMEM((ys, levels, bands, rows), jnp.bfloat16),
                pltpu.VMEM((ys, 4 * levels, bands), jnp.float32),
                dma((xs, levels)), dma((xs, levels)), dma((xs,)), dma((xs,)),
                dma((ys, levels)), dma((ys, levels)), dma((ys,)), dma((ys,)),
            ],
            compiler_params=pltpu.CompilerParams(collective_id=0, has_side_effects=True),
        )(field, edge, table, ztable, weights)

        edge_got = edge_got.reshape(n_gy, 4, levels, bands)
        low = lax.dynamic_index_in_dim(edge_got, me_y, 0, keepdims=False)
        high = lax.dynamic_index_in_dim(edge_got, (me_y + 1) % n_gy, 0, keepdims=False)
        low, high = low.transpose(0, 2, 1), high.transpose(0, 2, 1)
        spectra_zone = blend_zone(high[2], high[3], low[0], low[1], EXT_ZONE)

        spectra = jnp.zeros((bands, levels, ny), jnp.float32)
        for shift in range(n_gy):
            full = got[shift].transpose(1, 0, 2).astype(jnp.float32)
            source = (me_y + n_gy - shift) % n_gy
            spectra = lax.dynamic_update_slice(spectra, full, (0, 0, source * rows))
        return spectra, spectra_zone

    return body


ROWS = 128
GROUP = 16


def host_weights(zone_count):
    t = (np.arange(zone_count, dtype=np.float32) + np.float32(1)) / np.float32(zone_count + 1.0)
    two, three, one = np.float32(2), np.float32(3), np.float32(1)
    cube, square = t * t * t, t * t
    return (two * cube - three * square + one, cube - two * square + t,
            three * square - two * cube, cube - square)


def unit_circle(product, length):
    quarter = length / 4.0
    turns = jnp.floor(product * (4.0 / length) + 0.5)
    theta = (product - turns * quarter) * (2.0 * math.pi / length)
    turns = turns - 4.0 * jnp.floor(turns * 0.25)
    z = theta * theta
    sin = theta * (1.0 + z * (-1.0 / 6 + z * (1.0 / 120 + z * (-1.0 / 5040 + z * (1.0 / 362880)))))
    cos = 1.0 + z * (-0.5 + z * (1.0 / 24 + z * (-1.0 / 720 + z * (1.0 / 40320 - z * (1.0 / 3628800)))))
    odd = (turns == 1.0) | (turns == 3.0)
    c, s = jnp.where(odd, sin, cos), jnp.where(odd, cos, sin)
    c = jnp.where((turns == 1.0) | (turns == 2.0), -c, c)
    s = jnp.where(turns >= 2.0, -s, s)
    return c, s


def fused_kernel(n_gx, n_gy, field_ref, out_ref, zone_ref,
                 own, xgot, got, send, tab, ztab, pq, cs, acc, esum, esend, egot,
                 ls, xs, xr, zs, zr, fs, fr, *, depth, lag):
    levels, rows, cols = field_ref.shape
    bands = got.shape[3]
    nblk = rows // ROWS
    size = n_gy * bands
    nx = n_gx * cols
    length = nx + EXT_ZONE
    me_x, me_y = lax.axis_index("gx"), lax.axis_index("gy")
    chunks = levels * nblk
    order = sorted(range(1, n_gy), key=lambda shift: abs(2 * shift - n_gy))

    def peer_x(shift):
        return {"gx": lax.rem(me_x + n_gx - shift, n_gx)}

    def peer_y(shift):
        return {"gy": lax.rem(me_y + shift, n_gy)}

    def source_y(shift):
        return lax.rem(me_y + n_gy - shift, n_gy)

    barrier = pltpu.get_barrier_semaphore()
    for shift in range(1, n_gx):
        pl.semaphore_signal(barrier, inc=1, device_id=peer_x(shift), device_id_type=MESH)
    for shift in range(1, n_gy):
        pl.semaphore_signal(barrier, inc=1, device_id=peer_y(shift), device_id_type=MESH)

    def place(i, owner):
        ahead = jnp.where(owner == n_gy - 1, nblk - 1, 0)
        return lax.rem(i // levels + ahead, nblk), lax.rem(i, levels)

    def load(i):
        blk, level = place(i, me_y)
        at = pl.ds(pl.multiple_of(blk * ROWS, ROWS), ROWS)
        return pltpu.make_async_copy(field_ref.at[level, at], own.at[level, at], ls.at[blk, level])

    def rows_x(shift, i):
        blk, level = place(i, me_y)
        at = pl.ds(pl.multiple_of(blk * ROWS, ROWS), ROWS)
        return pltpu.make_async_remote_copy(
            src_ref=field_ref.at[level, at], dst_ref=xgot.at[shift - 1, level, at],
            send_sem=xs.at[shift - 1, blk, level], recv_sem=xr.at[shift - 1, blk, level],
            device_id=peer_x(shift), device_id_type=MESH)

    def spec_y(shift, i, source):
        blk, level = place(i, source)
        return pltpu.make_async_remote_copy(
            src_ref=send.at[shift - 1, blk, level], dst_ref=got.at[source, blk, level],
            send_sem=zs.at[shift - 1, blk, level], recv_sem=zr.at[shift - 1, blk, level],
            device_id=peer_y(shift), device_id_type=MESH)

    def edge_y(side, shift):
        return pltpu.make_async_remote_copy(
            src_ref=esend.at[shift], dst_ref=egot.at[side],
            send_sem=fs.at[shift - 1], recv_sem=fr.at[side],
            device_id=peer_y(shift), device_id_type=MESH)

    @pl.loop(0, chunks)
    def _(i):
        load(i).start()

    pl.semaphore_wait(barrier, n_gx + n_gy - 2)

    @pl.loop(0, depth)
    def _(i):
        for shift in range(1, n_gx):
            rows_x(shift, i).start()

    norm = 1.0 / math.sqrt(length)
    ngroup = size // GROUP
    g = lax.broadcasted_iota(jnp.int32, (ngroup, 1), 0) * GROUP
    shift_at = g // bands
    first = lax.rem(me_y + shift_at, n_gy) * (n_gx * bands) + me_x * bands + (g - shift_at * bands)
    is_cos = first < nx // 2
    number = jnp.where(is_cos, first, first - (nx // 2 - 1)).astype(jnp.float32)
    step = lax.broadcasted_iota(jnp.int32, (GROUP, 1), 0).astype(jnp.float32)

    def factors(column):
        c, s = unit_circle(number * column, length)
        p, q = jnp.where(is_cos, c, -s), jnp.where(is_cos, s, c)
        c, s = unit_circle(step * column, length)
        return p, q, c * norm, s * norm

    def expand(write, width):
        @pl.loop(0, ngroup // 8)
        def _(k):
            at = pl.ds(pl.multiple_of(k * 8, 8), 8)
            for r in range(8):
                p, q = pq[0, at, :width][r:r + 1], pq[1, at, :width][r:r + 1]
                write(pl.multiple_of((k * 8 + r) * GROUP, GROUP), p * cs[0, :, :width] - q * cs[1, :, :width])

    for at in range(n_gx):
        base = (lax.rem(me_x + at, n_gx) * cols).astype(jnp.float32)
        column = lax.broadcasted_iota(jnp.int32, (1, cols), 1).astype(jnp.float32) + base
        pq[0], pq[1], cs[0], cs[1] = factors(column)

        def write(k, value, at=at):
            tab[at, pl.ds(k, GROUP), :] = value.astype(jnp.bfloat16)

        expand(write, cols)
    lane = lax.broadcasted_iota(jnp.int32, (1, LANES), 1)
    p, q, c, s = factors(lane.astype(jnp.float32) + float(nx))
    pq[0, :, :LANES], pq[1, :, :LANES], cs[0, :, :LANES], cs[1, :, :LANES] = p, q, c, s

    def write_zone(k, value):
        ztab[pl.ds(k, GROUP), :] = jnp.where(lane < EXT_ZONE, value, 0.0).astype(jnp.bfloat16)

    expand(write_zone, LANES)

    t = jnp.minimum(lane + 1, EXT_ZONE).astype(jnp.float32) / (EXT_ZONE + 1.0)
    cube, square = t * t * t, t * t
    weight_a = 2.0 * cube - 3.0 * square + 1.0
    weight_b = cube - 2.0 * square + t
    weight_c = -2.0 * cube + 3.0 * square
    weight_d = cube - square
    tangent = EXT_ZONE + 1.0
    tail = cols - LANES

    def zone_of(parts):
        first = second = last = before = 0.0
        for at, part in enumerate(parts):
            owner = lax.rem(me_x + at, n_gx)
            is_first = jnp.where(owner == 0, 1.0, 0.0)
            is_last = jnp.where(owner == n_gx - 1, 1.0, 0.0)
            head = part[:, :LANES].astype(jnp.float32)
            rear = part[:, tail:].astype(jnp.float32)
            first += is_first * head[:, 0:1]
            second += is_first * head[:, 1:2]
            before += is_last * rear[:, LANES - 2:LANES - 1]
            last += is_last * rear[:, LANES - 1:LANES]
        zone = (last * weight_a + (tangent * (last - before)) * weight_b
                + first * weight_c + (tangent * (second - first)) * weight_d)
        return zone.astype(jnp.bfloat16)

    def dot(a, b):
        return lax.dot_general(a, b, NT, preferred_element_type=jnp.float32)

    def arrive(i):
        for shift in range(n_gy):
            source = source_y(shift)
            blk, level = place(i, source)
            if shift:
                spec_y(shift, i, source).wait_recv()
            out_ref[source * nblk + blk, pl.ds(level, bands, stride=levels), :] = (
                got[source, blk, level].astype(jnp.float32))

    def split(i):
        blk, level = place(i, me_y)
        at = pl.ds(pl.multiple_of(blk * ROWS, ROWS), ROWS)
        return blk, level, at

    def own_part(i):
        blk, level, at = split(i)
        acc[...] = dot(tab[0], own[level, at, :])

    def compute(i):
        blk, level, at = split(i)
        parts = [own[level, at, :]] + [xgot[x, level, at, :] for x in range(n_gx - 1)]
        total = acc[...] + dot(ztab[...], zone_of(parts))
        for x in range(1, n_gx):
            total += dot(tab[x], parts[x])
        got[me_y, blk, level] = total[:bands].astype(jnp.bfloat16)
        for shift in range(1, n_gy):
            send[shift - 1, blk, level] = total[shift * bands:(shift + 1) * bands].astype(jnp.bfloat16)

    def edges():
        top = me_y == 0
        row0 = pl.multiple_of(jnp.where(top, 0, rows - 16), 16)
        parts = [own[:, pl.ds(row0, 16), :].reshape(levels * 16, cols)]
        parts += [xgot[x, :, pl.ds(row0, 16), :].reshape(levels * 16, cols) for x in range(n_gx - 1)]
        total = dot(zone_of(parts), ztab[...])
        for x, part in enumerate(parts):
            total += dot(part, tab[x])
        esum[...] = total
        for pair in range(2):
            for level in range(levels):
                upper = esum[level * 16 + pair:level * 16 + pair + 1, :]
                lower = esum[level * 16 + 14 + pair:level * 16 + 15 + pair, :]
                line = jnp.where(top, upper, lower)
                for shift in range(n_gy):
                    esend[shift, pair, level:level + 1, :] = line[:, shift * bands:(shift + 1) * bands]
        for side, owner in ((0, 0), (1, n_gy - 1)):
            @pl.when(me_y == owner)
            def _(side=side):
                egot[side] = esend[0]
                for shift in range(1, n_gy):
                    edge_y(side, shift).start()

    seam = (me_y == 0) | (me_y == n_gy - 1)

    @pl.loop(0, chunks)
    def _(i):
        load(i).wait()
        own_part(i)
        for shift in range(1, n_gx):
            rows_x(shift, i).wait_recv()

        @pl.when(i + depth < chunks)
        def _():
            for shift in range(1, n_gx):
                rows_x(shift, i + depth).start()

        compute(i)
        for shift in order:
            spec_y(shift, i, me_y).start()

        @pl.when(seam & (i == levels - 1))
        def _():
            edges()

        @pl.when(i >= lag)
        def _():
            arrive(i - lag)

    for side, owner in ((0, 0), (1, n_gy - 1)):
        @pl.when(me_y != owner)
        def _(side=side):
            edge_y(side, 1).wait_recv()

        @pl.when(me_y == owner)
        def _(side=side):
            for shift in range(1, n_gy):
                edge_y(side, shift).wait_send()

    wa, wb, wc, wd = host_weights(EXT_ZONE)
    slope_start = tangent * (egot[1, 1] - egot[1, 0])
    slope_end = tangent * (egot[0, 1] - egot[0, 0])
    for j in range(EXT_ZONE):
        zone_ref[j] = (egot[1, 1] * float(wa[j]) + slope_start * float(wb[j])
                       + egot[0, 0] * float(wc[j]) + slope_end * float(wd[j]))

    @pl.loop(chunks - lag, chunks)
    def _(i):
        arrive(i)

    @pl.loop(0, chunks)
    def _(i):
        for shift in range(1, n_gx):
            rows_x(shift, i).wait_send()
        for shift in range(1, n_gy):
            spec_y(shift, i, me_y).wait_send()


def make_fused_body(mesh):
    n_gx, n_gy = mesh.shape["gx"], mesh.shape["gy"]

    def body(field):
        levels, rows, cols = field.shape
        bands = cols // n_gy
        nblk, ny, size = rows // ROWS, rows * n_gy, n_gy * bands
        xs, ys = n_gx - 1, n_gy - 1
        vmem, dma = pl.BlockSpec(memory_space=pltpu.VMEM), pltpu.SemaphoreType.DMA
        bf16, f32 = jnp.bfloat16, jnp.float32
        spectra, zone = pl.pallas_call(
            functools.partial(fused_kernel, n_gx, n_gy, depth=DEPTH, lag=LAG),
            out_shape=(
                jax.ShapeDtypeStruct((n_gy * nblk, bands * levels, ROWS), f32),
                jax.ShapeDtypeStruct((EXT_ZONE, levels, bands), f32),
            ),
            in_specs=[pl.BlockSpec(memory_space=pltpu.HBM)],
            out_specs=(vmem, vmem),
            scratch_shapes=[
                pltpu.VMEM((levels, rows, cols), bf16),
                pltpu.VMEM((xs, levels, rows, cols), bf16),
                pltpu.VMEM((n_gy, nblk, levels, bands, ROWS), bf16),
                pltpu.VMEM((ys, nblk, levels, bands, ROWS), bf16),
                pltpu.VMEM((n_gx, size, cols), bf16),
                pltpu.VMEM((size, LANES), bf16),
                pltpu.VMEM((2, size // GROUP, cols), f32),
                pltpu.VMEM((2, GROUP, cols), f32),
                pltpu.VMEM((size, ROWS), f32),
                pltpu.VMEM((levels * 16, size), f32),
                pltpu.VMEM((n_gy, 2, levels, bands), f32),
                pltpu.VMEM((2, 2, levels, bands), f32),
                dma((nblk, levels)),
                dma((xs, nblk, levels)), dma((xs, nblk, levels)),
                dma((ys, nblk, levels)), dma((ys, nblk, levels)),
                dma((ys,)), dma((2,)),
            ],
            compiler_params=pltpu.CompilerParams(
                collective_id=0, has_side_effects=True, vmem_limit_bytes=VMEM_LIMIT),
        )(pltpu.with_memory_space_constraint(field, pltpu.HBM))
        spectra = pl.pallas_call(
            store_kernel,
            out_shape=jax.ShapeDtypeStruct((bands * levels, ny), f32),
            in_specs=[vmem],
            out_specs=pl.BlockSpec(memory_space=pl.ANY),
            scratch_shapes=[dma((n_gy * nblk,))],
            compiler_params=pltpu.CompilerParams(vmem_limit_bytes=VMEM_LIMIT_STORE),
        )(spectra)
        return spectra.reshape(bands, levels, ny), zone.transpose(2, 1, 0)

    return body


def store_kernel(tile_ref, out_ref, sem):
    copies = [
        pltpu.make_async_copy(tile_ref.at[b], out_ref.at[:, pl.ds(b * ROWS, ROWS)], sem.at[b])
        for b in range(tile_ref.shape[0])
    ]
    for copy in copies:
        copy.start()
    for copy in copies:
        copy.wait()


VMEM_LIMIT_STORE = 16 * 2**20
DEPTH, LAG = 4, 3
VMEM_LIMIT = 36 * 2**20


def fits(mesh, shape):
    n_gx, n_gy = mesh.shape["gx"], mesh.shape["gy"]
    levels = shape[0] // (mesh.shape["member"] * mesh.shape["lev"])
    rows, cols = shape[1] // n_gy, shape[2] // n_gx
    bands = cols // n_gy
    return (n_gx > 1 and n_gy > 1 and rows % ROWS == 0 and cols % LANES == 0 and bands % GROUP == 0 and n_gy * bands % (8 * GROUP) == 0
            and (cols * n_gx // 2) % bands == 0 and levels % 8 == 0 and levels * rows // ROWS > DEPTH)


def solution(mesh):
    def program(field):
        body = make_fused_body(mesh) if fits(mesh, field.shape) else make_plain_body(mesh)
        return jax.shard_map(
            body,
            mesh=mesh,
            in_specs=(P(("member", "lev"), "gy", "gx"),),
            out_specs=(
                P(("gy", "gx"), ("member", "lev"), None),
                P(("gy", "gx"), ("member", "lev"), None),
            ),
            check_vma=False,
        )(field)

    return program
```

```python
import functools
import math

import jax
import jax.numpy as jnp
import numpy as np
from jax import lax
from jax.experimental import pallas as pl
from jax.experimental.pallas import tpu as pltpu
from jax.sharding import PartitionSpec as P

EXT_ZONE = 11
LANES = 128
NT = (((1,), (1,)), ((), ()))
MESH = pl.DeviceIdType.MESH


def blend_weights(zone_count):
    steps = (jnp.arange(zone_count, dtype=jnp.int32) + 1).astype(jnp.float32) / (zone_count + 1.0)
    weight_a = 2.0 * steps**3 - 3.0 * steps**2 + 1.0
    weight_b = steps**3 - 2.0 * steps**2 + steps
    weight_c = -2.0 * steps**3 + 3.0 * steps**2
    weight_d = steps**3 - steps**2
    return weight_a, weight_b, weight_c, weight_d


def blend_zone(second_last, last_value, first_value, second_value, zone_count):
    weight_a, weight_b, weight_c, weight_d = blend_weights(zone_count)
    tangent_scale = zone_count + 1.0
    slope_start = tangent_scale * (last_value - second_last)
    slope_end = tangent_scale * (second_value - first_value)
    return (
        last_value[..., None] * weight_a
        + slope_start[..., None] * weight_b
        + first_value[..., None] * weight_c
        + slope_end[..., None] * weight_d
    )


def wave_factors(coeff0, group, column, wave_count, length):
    number0 = jnp.where(coeff0 < wave_count, coeff0, coeff0 - wave_count + 1)
    scale = 2.0 * math.pi / length
    phase0 = (number0[:, None] * column[None, :] % length).astype(jnp.float32) * scale
    cos0, sin0 = jnp.cos(phase0), jnp.sin(phase0)
    is_cosine = (coeff0 < wave_count)[:, None]
    p, q = jnp.where(is_cosine, cos0, -sin0), jnp.where(is_cosine, sin0, cos0)
    step = jnp.arange(group, dtype=jnp.int32)
    phase = (step[:, None] * column[None, :] % length).astype(jnp.float32) * scale
    norm = 1.0 / math.sqrt(length)
    return p, q, jnp.cos(phase) * norm, jnp.sin(phase) * norm


def kernel(n_gx, n_gy, field_ref, edge_ref, table_ref, ztable_ref, weight_ref,
           out_ref, out_edge_ref, xgot, xedge, send, esend, xs, xr, es, er, zs, zr, ts, tr):
    levels, rows, cols = field_ref.shape
    bands = table_ref.shape[2]
    me_x, me_y = lax.axis_index("gx"), lax.axis_index("gy")

    def peer_x(shift):
        return {"gx": lax.rem(me_x + n_gx - shift, n_gx)}

    def peer_y(shift):
        return {"gy": lax.rem(me_y + shift, n_gy)}

    barrier = pltpu.get_barrier_semaphore()
    for shift in range(1, n_gx):
        pl.semaphore_signal(barrier, inc=1, device_id=peer_x(shift), device_id_type=MESH)
    for shift in range(1, n_gy):
        pl.semaphore_signal(barrier, inc=1, device_id=peer_y(shift), device_id_type=MESH)
    pl.semaphore_wait(barrier, n_gx + n_gy - 2)

    def edge_x(shift):
        return pltpu.make_async_remote_copy(
            src_ref=edge_ref, dst_ref=xedge.at[shift - 1], send_sem=es.at[shift - 1],
            recv_sem=er.at[shift - 1], device_id=peer_x(shift), device_id_type=MESH)

    def rows_x(shift, level):
        return pltpu.make_async_remote_copy(
            src_ref=field_ref.at[level], dst_ref=xgot.at[shift - 1, level],
            send_sem=xs.at[shift - 1, level], recv_sem=xr.at[shift - 1, level],
            device_id=peer_x(shift), device_id_type=MESH)

    def edge_y(shift):
        return pltpu.make_async_remote_copy(
            src_ref=esend.at[shift - 1], dst_ref=out_edge_ref.at[shift], send_sem=ts.at[shift - 1],
            recv_sem=tr.at[shift - 1], device_id=peer_y(shift), device_id_type=MESH)

    def spec_y(shift, level):
        return pltpu.make_async_remote_copy(
            src_ref=send.at[shift - 1, level], dst_ref=out_ref.at[shift, level],
            send_sem=zs.at[shift - 1, level], recv_sem=zr.at[shift - 1, level],
            device_id=peer_y(shift), device_id_type=MESH)

    for shift in range(1, n_gx):
        edge_x(shift).start()

    @pl.loop(0, levels)
    def _(level):
        for shift in range(1, n_gx):
            rows_x(shift, level).start()

    tail = (cols - 1) // LANES * LANES

    def zone_of(parts):
        first = second = last = before = 0.0
        for at, part in enumerate(parts):
            owner = lax.rem(me_x + at, n_gx)
            is_first = jnp.where(owner == 0, 1.0, 0.0)
            is_last = jnp.where(owner == n_gx - 1, 1.0, 0.0)
            head = part[:, :min(LANES, cols)].astype(jnp.float32)
            rear = part[:, tail:].astype(jnp.float32)
            first += is_first * head[:, 0:1]
            second += is_first * head[:, 1:2]
            before += is_last * rear[:, cols - 2 - tail:cols - 1 - tail]
            last += is_last * rear[:, cols - 1 - tail:cols - tail]
        tangent = EXT_ZONE + 1.0
        zone = (last * weight_ref[0:1, :] + (tangent * (last - before)) * weight_ref[1:2, :]
                + first * weight_ref[2:3, :] + (tangent * (second - first)) * weight_ref[3:4, :])
        return zone.astype(jnp.bfloat16)

    def dot(a, b):
        return lax.dot_general(a, b, NT, preferred_element_type=jnp.float32)

    for shift in range(1, n_gx):
        edge_x(shift).wait_recv()
    parts = [edge_ref[...]] + [xedge[at] for at in range(n_gx - 1)]
    zone = zone_of(parts)
    for shift in range(n_gy):
        total = dot(zone, ztable_ref[shift])
        for at, part in enumerate(parts):
            total += dot(part, table_ref[at, shift])
        if shift == 0:
            out_edge_ref[0] = total
        else:
            esend[shift - 1] = total
            edge_y(shift).start()

    merged = bands % 16 == 0

    @pl.loop(0, levels)
    def _(level):
        for shift in range(1, n_gx):
            rows_x(shift, level).wait_recv()
        parts = [field_ref[level]] + [xgot[at, level] for at in range(n_gx - 1)]
        zone = zone_of(parts)
        if merged:
            size = n_gy * bands
            total = dot(ztable_ref[...].reshape(size, LANES), zone)
            for at, part in enumerate(parts):
                total += dot(table_ref[at].reshape(size, cols), part)
            pieces = [total[s * bands:(s + 1) * bands] for s in range(n_gy)]
        else:
            pieces = []
            for shift in range(n_gy):
                total = dot(ztable_ref[shift], zone)
                for at, part in enumerate(parts):
                    total += dot(table_ref[at, shift], part)
                pieces.append(total)
        for shift in range(n_gy):
            piece = pieces[shift].astype(jnp.bfloat16)
            if shift == 0:
                out_ref[0, level] = piece
            else:
                send[shift - 1, level] = piece
        for shift in range(1, n_gy):
            spec_y(shift, level).start()

    for shift in range(1, n_gx):
        edge_x(shift).wait_send()
    for shift in range(1, n_gy):
        edge_y(shift).wait()

    @pl.loop(0, levels)
    def _(level):
        for shift in range(1, n_gx):
            rows_x(shift, level).wait_send()
        for shift in range(1, n_gy):
            spec_y(shift, level).wait()


def make_plain_body(mesh):
    n_gx, n_gy = mesh.shape["gx"], mesh.shape["gy"]

    def body(field):
        levels, rows, cols = field.shape
        nx, ny = cols * n_gx, rows * n_gy
        length = nx + EXT_ZONE
        me_x, me_y = lax.axis_index("gx"), lax.axis_index("gy")
        bands = nx // (n_gx * n_gy)
        assert (nx // 2) % bands == 0
        group = 16 if bands % 16 == 0 else bands

        at = jnp.arange(nx + LANES, dtype=jnp.int32)
        column = jnp.where(at < nx, (at + me_x * cols) % nx, at)
        shift_at = jnp.arange(n_gy, dtype=jnp.int32)[:, None]
        coeff = ((me_y + shift_at) % n_gy) * (n_gx * bands) + me_x * bands
        coeff = (coeff + jnp.arange(0, bands, group, dtype=jnp.int32)[None, :]).reshape(-1)
        factors = wave_factors(coeff, group, column, nx // 2, length)
        p, q, c, s = lax.optimization_barrier(factors)

        def expand(lo, hi):
            full = p[:, None, lo:hi] * c[None, :, lo:hi] - q[:, None, lo:hi] * s[None, :, lo:hi]
            return full.astype(jnp.bfloat16).reshape(n_gy, bands, hi - lo)

        table = jnp.stack([expand(i * cols, (i + 1) * cols) for i in range(n_gx)])
        ztable = expand(nx, nx + LANES)
        ztable = jnp.where(jnp.arange(LANES) < EXT_ZONE, ztable, jnp.zeros_like(ztable))
        weights = jnp.pad(jnp.stack(blend_weights(EXT_ZONE)), ((0, 4), (0, LANES - EXT_ZONE)))
        edge = jnp.concatenate([field[:, :2], field[:, rows - 2:]], axis=1)
        edge = edge.transpose(1, 0, 2).reshape(4 * levels, cols)

        vmem = pl.BlockSpec(memory_space=pltpu.VMEM)
        dma = pltpu.SemaphoreType.DMA
        xs, ys = n_gx - 1, n_gy - 1
        got, edge_got = pl.pallas_call(
            functools.partial(kernel, n_gx, n_gy),
            out_shape=(
                jax.ShapeDtypeStruct((n_gy, levels, bands, rows), jnp.bfloat16),
                jax.ShapeDtypeStruct((n_gy, 4 * levels, bands), jnp.float32),
            ),
            in_specs=[vmem] * 5,
            out_specs=(vmem, vmem),
            scratch_shapes=[
                pltpu.VMEM((xs, levels, rows, cols), jnp.bfloat16),
                pltpu.VMEM((xs, 4 * levels, cols), jnp.bfloat16),
                pltpu.VMEM((ys, levels, bands, rows), jnp.bfloat16),
                pltpu.VMEM((ys, 4 * levels, bands), jnp.float32),
                dma((xs, levels)), dma((xs, levels)), dma((xs,)), dma((xs,)),
                dma((ys, levels)), dma((ys, levels)), dma((ys,)), dma((ys,)),
            ],
            compiler_params=pltpu.CompilerParams(collective_id=0, has_side_effects=True),
        )(field, edge, table, ztable, weights)

        edge_got = edge_got.reshape(n_gy, 4, levels, bands)
        low = lax.dynamic_index_in_dim(edge_got, me_y, 0, keepdims=False)
        high = lax.dynamic_index_in_dim(edge_got, (me_y + 1) % n_gy, 0, keepdims=False)
        low, high = low.transpose(0, 2, 1), high.transpose(0, 2, 1)
        spectra_zone = blend_zone(high[2], high[3], low[0], low[1], EXT_ZONE)

        spectra = jnp.zeros((bands, levels, ny), jnp.float32)
        for shift in range(n_gy):
            full = got[shift].transpose(1, 0, 2).astype(jnp.float32)
            source = (me_y + n_gy - shift) % n_gy
            spectra = lax.dynamic_update_slice(spectra, full, (0, 0, source * rows))
        return spectra, spectra_zone

    return body


ROWS = 128
GROUP = 16


def host_weights(zone_count):
    t = (np.arange(zone_count, dtype=np.float32) + np.float32(1)) / np.float32(zone_count + 1.0)
    two, three, one = np.float32(2), np.float32(3), np.float32(1)
    cube, square = t * t * t, t * t
    return (two * cube - three * square + one, cube - two * square + t,
            three * square - two * cube, cube - square)


def unit_circle(product, length):
    quarter = length / 4.0
    turns = jnp.floor(product * (4.0 / length) + 0.5)
    theta = (product - turns * quarter) * (2.0 * math.pi / length)
    turns = turns - 4.0 * jnp.floor(turns * 0.25)
    z = theta * theta
    sin = theta * (1.0 + z * (-1.0 / 6 + z * (1.0 / 120 + z * (-1.0 / 5040 + z * (1.0 / 362880)))))
    cos = 1.0 + z * (-0.5 + z * (1.0 / 24 + z * (-1.0 / 720 + z * (1.0 / 40320 - z * (1.0 / 3628800)))))
    odd = (turns == 1.0) | (turns == 3.0)
    c, s = jnp.where(odd, sin, cos), jnp.where(odd, cos, sin)
    c = jnp.where((turns == 1.0) | (turns == 2.0), -c, c)
    s = jnp.where(turns >= 2.0, -s, s)
    return c, s


def fused_kernel(n_gx, n_gy, field_ref, out_ref, zone_ref,
                 own, xgot, got, send, tab, ztab, pq, cs, acc, esum, esend, egot,
                 ls, xs, xr, zs, zr, fs, fr, far, *, depth, lag):
    levels, rows, cols = field_ref.shape
    bands = got.shape[3]
    nblk = rows // ROWS
    size = n_gy * bands
    nx = n_gx * cols
    length = nx + EXT_ZONE
    me_x, me_y = lax.axis_index("gx"), lax.axis_index("gy")
    chunks = levels * nblk

    def peer_x(shift):
        return {"gx": lax.rem(me_x + n_gx - shift, n_gx)}

    def peer_y(shift):
        return {"gy": lax.rem(me_y + shift, n_gy)}

    def turn(k):
        up, down = n_gy - 1 - k, k
        up = jnp.where(up > me_y, up, up - 1)
        down = jnp.where(down < me_y, down, down + 1)
        return lax.rem(jnp.where(2 * me_y < n_gy, up, down) - me_y + n_gy, n_gy)

    above, below = me_y < n_gy - 1, me_y > 0

    def tell(semaphore, up):
        pl.semaphore_signal(semaphore, inc=1, device_id={"gy": me_y + (1 if up else -1)},
                            device_id_type=MESH)

    barrier = pltpu.get_barrier_semaphore()
    for shift in range(1, n_gx):
        pl.semaphore_signal(barrier, inc=1, device_id=peer_x(shift), device_id_type=MESH)
    pl.when(above)(lambda: tell(barrier, True))
    pl.when(below)(lambda: tell(barrier, False))

    def vouch():
        pl.when(above & below)(lambda: tell(far.at[0], False))
        pl.when(above & below)(lambda: tell(far.at[1], True))

    def hear():
        for hop in range(n_gy - 2):
            @pl.when(me_y + hop < n_gy - 2)
            def _():
                pl.semaphore_wait(far.at[0], 1)
                pl.when(below)(lambda: tell(far.at[0], False))

            @pl.when(me_y - hop > 1)
            def _():
                pl.semaphore_wait(far.at[1], 1)
                pl.when(above)(lambda: tell(far.at[1], True))

    def place(i, owner):
        ahead = jnp.where(owner == n_gy - 1, nblk - 1, 0)
        return lax.rem(i // levels + ahead, nblk), lax.rem(i, levels)

    def lines(blk):
        return pl.ds(pl.multiple_of(blk * ROWS, ROWS), ROWS)

    def load(turn_at):
        blk, _ = place(turn_at * levels, me_y)
        at = lines(blk)
        return pltpu.make_async_copy(field_ref.at[:, at], own.at[:, at], ls.at[turn_at])

    def rows_x(shift, i):
        blk, level = place(i, me_y)
        at = lines(blk)
        return pltpu.make_async_remote_copy(
            src_ref=field_ref.at[level, at], dst_ref=xgot.at[shift - 1, level, at],
            send_sem=xs.at[shift - 1], recv_sem=xr.at[i],
            device_id=peer_x(shift), device_id_type=MESH)

    def rows_in(i):
        blk, level = place(i, me_y)
        ref = xgot.at[:, level, lines(blk)]
        return pltpu.make_async_remote_copy(
            src_ref=ref, dst_ref=ref, send_sem=xs.at[0], recv_sem=xr.at[i],
            device_id=peer_x(1), device_id_type=MESH)

    def spec_y(k, i):
        shift = turn(k)
        blk, level = place(i, me_y)
        return pltpu.make_async_remote_copy(
            src_ref=send.at[k, blk, level], dst_ref=got.at[me_y, blk, level],
            send_sem=zs, recv_sem=zr.at[i], device_id=peer_y(shift), device_id_type=MESH)

    def specs_in(i):
        return pltpu.make_async_remote_copy(
            src_ref=send.at[:, 0, 0], dst_ref=got.at[pl.ds(0, n_gy - 1), 0, 0],
            send_sem=zs, recv_sem=zr.at[i], device_id=peer_y(1), device_id_type=MESH)

    def edge_y(side, k):
        return pltpu.make_async_remote_copy(
            src_ref=esend.at[k], dst_ref=egot.at[side], send_sem=fs, recv_sem=fr.at[side],
            device_id=peer_y(turn(k)), device_id_type=MESH)

    def all_sent(ref, semaphore):
        pltpu.make_async_remote_copy(
            src_ref=ref, dst_ref=ref, send_sem=semaphore, recv_sem=fr.at[0],
            device_id=peer_y(1), device_id_type=MESH).wait_send()

    for turn_at in range(nblk):
        load(turn_at).start()

    pl.semaphore_wait(barrier, n_gx - 1 + above.astype(jnp.int32) + below.astype(jnp.int32))

    @pl.loop(0, depth)
    def _(i):
        for shift in range(1, n_gx):
            rows_x(shift, i).start()

    vouch()

    norm = 1.0 / math.sqrt(length)
    ngroup = size // GROUP
    g = lax.broadcasted_iota(jnp.int32, (ngroup, 1), 0) * GROUP
    block = g // bands
    owner = jnp.full((ngroup, 1), me_y, jnp.int32)
    for k in range(n_gy - 1):
        owner = jnp.where(block == k, lax.rem(me_y + turn(k), n_gy), owner)
    first = owner * (n_gx * bands) + me_x * bands + (g - block * bands)
    is_cos = first < nx // 2
    number = jnp.where(is_cos, first, first - (nx // 2 - 1)).astype(jnp.float32)
    step = lax.broadcasted_iota(jnp.int32, (GROUP, 1), 0).astype(jnp.float32)

    def factors(column):
        c, s = unit_circle(number * column, length)
        p, q = jnp.where(is_cos, c, -s), jnp.where(is_cos, s, c)
        c, s = unit_circle(step * column, length)
        return p, q, c * norm, s * norm

    def expand(write, width):
        @pl.loop(0, ngroup // 8)
        def _(k):
            at = pl.ds(pl.multiple_of(k * 8, 8), 8)
            for r in range(8):
                p, q = pq[0, at, :width][r:r + 1], pq[1, at, :width][r:r + 1]
                write(pl.multiple_of((k * 8 + r) * GROUP, GROUP), p * cs[0, :, :width] - q * cs[1, :, :width])

    for at in range(n_gx):
        base = (lax.rem(me_x + at, n_gx) * cols).astype(jnp.float32)
        column = lax.broadcasted_iota(jnp.int32, (1, cols), 1).astype(jnp.float32) + base
        pq[0], pq[1], cs[0], cs[1] = factors(column)

        def write(k, value, at=at):
            tab[at, pl.ds(k, GROUP), :] = value.astype(jnp.bfloat16)

        expand(write, cols)
    lane = lax.broadcasted_iota(jnp.int32, (1, LANES), 1)
    p, q, c, s = factors(lane.astype(jnp.float32) + float(nx))
    pq[0, :, :LANES], pq[1, :, :LANES], cs[0, :, :LANES], cs[1, :, :LANES] = p, q, c, s

    def write_zone(k, value):
        ztab[pl.ds(k, GROUP), :] = jnp.where(lane < EXT_ZONE, value, 0.0).astype(jnp.bfloat16)

    expand(write_zone, LANES)

    hear()

    t = jnp.minimum(lane + 1, EXT_ZONE).astype(jnp.float32) / (EXT_ZONE + 1.0)
    cube, square = t * t * t, t * t
    weight_a = 2.0 * cube - 3.0 * square + 1.0
    weight_b = cube - 2.0 * square + t
    weight_c = -2.0 * cube + 3.0 * square
    weight_d = cube - square
    tangent = EXT_ZONE + 1.0
    tail = cols - LANES

    def zone_of(parts):
        first = second = last = before = 0.0
        for at, part in enumerate(parts):
            owner = lax.rem(me_x + at, n_gx)
            is_first = jnp.where(owner == 0, 1.0, 0.0)
            is_last = jnp.where(owner == n_gx - 1, 1.0, 0.0)
            head = part[:, :LANES].astype(jnp.float32)
            rear = part[:, tail:].astype(jnp.float32)
            first += is_first * head[:, 0:1]
            second += is_first * head[:, 1:2]
            before += is_last * rear[:, LANES - 2:LANES - 1]
            last += is_last * rear[:, LANES - 1:LANES]
        zone = (last * weight_a + (tangent * (last - before)) * weight_b
                + first * weight_c + (tangent * (second - first)) * weight_d)
        return zone.astype(jnp.bfloat16)

    def dot(a, b):
        return lax.dot_general(a, b, NT, preferred_element_type=jnp.float32)

    def arrive(i):
        specs_in(i).wait_recv()
        for source in range(n_gy):
            blk, level = place(i, source)
            out_ref[source * nblk + blk, pl.ds(level, bands, stride=levels), :] = (
                got[source, blk, level].astype(jnp.float32))

    def split(i):
        blk, level = place(i, me_y)
        at = pl.ds(pl.multiple_of(blk * ROWS, ROWS), ROWS)
        return blk, level, at

    def own_part(i):
        blk, level, at = split(i)
        acc[...] = dot(tab[0], own[level, at, :])

    def compute(i):
        blk, level, at = split(i)
        parts = [own[level, at, :]] + [xgot[x, level, at, :] for x in range(n_gx - 1)]
        zone = zone_of(parts)
        for lo, hi in ((0, n_gy // 2), (n_gy // 2, n_gy)):
            at = pl.ds(lo * bands, (hi - lo) * bands)
            total = acc[at, :] + dot(ztab[at, :], zone)
            for x in range(1, n_gx):
                total += dot(tab[x, at, :], parts[x])
            for k in range(lo, hi):
                piece = total[(k - lo) * bands:(k - lo + 1) * bands].astype(jnp.bfloat16)
                if k == n_gy - 1:
                    got[me_y, blk, level] = piece
                else:
                    send[k, blk, level] = piece
                    spec_y(k, i).start()

    def edges():
        top = me_y == 0
        row0 = pl.multiple_of(jnp.where(top, 0, rows - 16), 16)
        parts = [own[:, pl.ds(row0, 16), :].reshape(levels * 16, cols)]
        parts += [xgot[x, :, pl.ds(row0, 16), :].reshape(levels * 16, cols) for x in range(n_gx - 1)]
        total = dot(zone_of(parts), ztab[...])
        for x, part in enumerate(parts):
            total += dot(part, tab[x])
        esum[...] = total
        for pair in range(2):
            for level in range(levels):
                upper = esum[level * 16 + pair:level * 16 + pair + 1, :]
                lower = esum[level * 16 + 14 + pair:level * 16 + 15 + pair, :]
                line = jnp.where(top, upper, lower)
                for k in range(n_gy):
                    esend[k, pair, level:level + 1, :] = line[:, k * bands:(k + 1) * bands]
        for side, owner in ((0, 0), (1, n_gy - 1)):
            @pl.when(me_y == owner)
            def _(side=side):
                egot[side] = esend[n_gy - 1]
                for k in range(n_gy - 1):
                    edge_y(side, k).start()

    seam = (me_y == 0) | (me_y == n_gy - 1)

    @pl.loop(0, chunks)
    def _(i):
        for turn_at in range(nblk):
            @pl.when(i == turn_at * levels)
            def _():
                load(turn_at).wait()

        own_part(i)
        rows_in(i).wait_recv()

        @pl.when(i + depth < chunks)
        def _():
            for shift in range(1, n_gx):
                rows_x(shift, i + depth).start()

        compute(i)

        @pl.when(seam & (i == levels - 1))
        def _():
            edges()

        @pl.when(i >= lag)
        def _():
            arrive(i - lag)

    for side, owner in ((0, 0), (1, n_gy - 1)):
        @pl.when(me_y != owner)
        def _(side=side):
            edge_y(side, 0).wait_recv()

    pl.when(seam)(lambda: all_sent(esend.at[pl.ds(0, n_gy - 1)], fs))
    wa, wb, wc, wd = host_weights(EXT_ZONE)
    slope_start = tangent * (egot[1, 1] - egot[1, 0])
    slope_end = tangent * (egot[0, 1] - egot[0, 0])
    for j in range(EXT_ZONE):
        zone_ref[j] = (egot[1, 1] * float(wa[j]) + slope_start * float(wb[j])
                       + egot[0, 0] * float(wc[j]) + slope_end * float(wd[j]))

    for shift in range(1, n_gx):
        all_sent(field_ref, xs.at[shift - 1])

    @pl.loop(chunks - lag, chunks)
    def _(i):
        arrive(i)

    all_sent(send, zs)


def make_fused_body(mesh):
    n_gx, n_gy = mesh.shape["gx"], mesh.shape["gy"]

    def body(field):
        levels, rows, cols = field.shape
        bands = cols // n_gy
        nblk, ny, size = rows // ROWS, rows * n_gy, n_gy * bands
        xs, ys = n_gx - 1, n_gy - 1
        vmem, dma = pl.BlockSpec(memory_space=pltpu.VMEM), pltpu.SemaphoreType.DMA
        bf16, f32 = jnp.bfloat16, jnp.float32
        spectra, zone = pl.pallas_call(
            functools.partial(fused_kernel, n_gx, n_gy, depth=DEPTH, lag=LAG),
            out_shape=(
                jax.ShapeDtypeStruct((n_gy * nblk, bands * levels, ROWS), f32),
                jax.ShapeDtypeStruct((EXT_ZONE, levels, bands), f32),
            ),
            in_specs=[pl.BlockSpec(memory_space=pltpu.HBM)],
            out_specs=(vmem, vmem),
            scratch_shapes=[
                pltpu.VMEM((levels, rows, cols), bf16),
                pltpu.VMEM((xs, levels, rows, cols), bf16),
                pltpu.VMEM((n_gy, nblk, levels, bands, ROWS), bf16),
                pltpu.VMEM((ys, nblk, levels, bands, ROWS), bf16),
                pltpu.VMEM((n_gx, size, cols), bf16),
                pltpu.VMEM((size, LANES), bf16),
                pltpu.VMEM((2, size // GROUP, cols), f32),
                pltpu.VMEM((2, GROUP, cols), f32),
                pltpu.VMEM((size, ROWS), f32),
                pltpu.VMEM((levels * 16, size), f32),
                pltpu.VMEM((n_gy, 2, levels, bands), f32),
                pltpu.VMEM((2, 2, levels, bands), f32),
                dma((nblk,)), dma((xs,)), dma((levels * nblk,)), dma, dma((levels * nblk,)),
                dma, dma((2,)), pltpu.SemaphoreType.REGULAR((2,)),
            ],
            compiler_params=pltpu.CompilerParams(
                collective_id=0, has_side_effects=True, vmem_limit_bytes=VMEM_LIMIT),
        )(pltpu.with_memory_space_constraint(field, pltpu.HBM))
        spectra, zone = pl.pallas_call(
            store_kernel,
            out_shape=(
                jax.ShapeDtypeStruct((bands * levels, ny), f32),
                jax.ShapeDtypeStruct(zone.shape, f32),
            ),
            in_specs=[vmem, vmem],
            out_specs=(pl.BlockSpec(memory_space=pl.ANY),) * 2,
            scratch_shapes=[dma((n_gy * nblk + 1,))],
            compiler_params=pltpu.CompilerParams(vmem_limit_bytes=VMEM_LIMIT_STORE),
        )(spectra, zone)
        return spectra.reshape(bands, levels, ny), zone.transpose(2, 1, 0)

    return body


def store_kernel(tile_ref, zone_ref, out_ref, zone_out_ref, sem):
    count = tile_ref.shape[0]
    copies = [
        pltpu.make_async_copy(tile_ref.at[b], out_ref.at[:, pl.ds(b * ROWS, ROWS)], sem.at[b])
        for b in range(count)
    ]
    copies.append(pltpu.make_async_copy(zone_ref, zone_out_ref, sem.at[count]))
    for copy in copies:
        copy.start()
    for copy in copies:
        copy.wait()


VMEM_LIMIT_STORE = 16 * 2**20
DEPTH = 4
LAG = 6
VMEM_LIMIT = 36 * 2**20


def fits(mesh, shape):
    n_gx, n_gy = mesh.shape["gx"], mesh.shape["gy"]
    levels = shape[0] // (mesh.shape["member"] * mesh.shape["lev"])
    rows, cols = shape[1] // n_gy, shape[2] // n_gx
    bands = cols // n_gy
    return (n_gx > 1 and n_gy > 1 and rows % ROWS == 0 and cols % LANES == 0 and bands % GROUP == 0 and n_gy * bands % (8 * GROUP) == 0
            and (cols * n_gx // 2) % bands == 0 and levels % 8 == 0 and levels * rows // ROWS > DEPTH)


def solution(mesh):
    def program(field):
        body = make_fused_body(mesh) if fits(mesh, field.shape) else make_plain_body(mesh)
        return jax.shard_map(
            body,
            mesh=mesh,
            in_specs=(P(("member", "lev"), "gy", "gx"),),
            out_specs=(
                P(("gy", "gx"), ("member", "lev"), None),
                P(("gy", "gx"), ("member", "lev"), None),
            ),
            check_vma=False,
        )(field)

    return program
```

```python
import functools
import math

import jax
import jax.numpy as jnp
import numpy as np
from jax import lax
from jax.experimental import pallas as pl
from jax.experimental.pallas import tpu as pltpu
from jax.sharding import PartitionSpec as P

EXT_ZONE = 11
LANES = 128
NT = (((1,), (1,)), ((), ()))
MESH = pl.DeviceIdType.MESH


def blend_weights(zone_count):
    steps = (jnp.arange(zone_count, dtype=jnp.int32) + 1).astype(jnp.float32) / (zone_count + 1.0)
    weight_a = 2.0 * steps**3 - 3.0 * steps**2 + 1.0
    weight_b = steps**3 - 2.0 * steps**2 + steps
    weight_c = -2.0 * steps**3 + 3.0 * steps**2
    weight_d = steps**3 - steps**2
    return weight_a, weight_b, weight_c, weight_d


def blend_zone(second_last, last_value, first_value, second_value, zone_count):
    weight_a, weight_b, weight_c, weight_d = blend_weights(zone_count)
    tangent_scale = zone_count + 1.0
    slope_start = tangent_scale * (last_value - second_last)
    slope_end = tangent_scale * (second_value - first_value)
    return (
        last_value[..., None] * weight_a
        + slope_start[..., None] * weight_b
        + first_value[..., None] * weight_c
        + slope_end[..., None] * weight_d
    )


def wave_factors(coeff0, group, column, wave_count, length):
    number0 = jnp.where(coeff0 < wave_count, coeff0, coeff0 - wave_count + 1)
    scale = 2.0 * math.pi / length
    phase0 = (number0[:, None] * column[None, :] % length).astype(jnp.float32) * scale
    cos0, sin0 = jnp.cos(phase0), jnp.sin(phase0)
    is_cosine = (coeff0 < wave_count)[:, None]
    p, q = jnp.where(is_cosine, cos0, -sin0), jnp.where(is_cosine, sin0, cos0)
    step = jnp.arange(group, dtype=jnp.int32)
    phase = (step[:, None] * column[None, :] % length).astype(jnp.float32) * scale
    norm = 1.0 / math.sqrt(length)
    return p, q, jnp.cos(phase) * norm, jnp.sin(phase) * norm


def kernel(n_gx, n_gy, field_ref, edge_ref, table_ref, ztable_ref, weight_ref,
           out_ref, out_edge_ref, xgot, xedge, send, esend, xs, xr, es, er, zs, zr, ts, tr):
    levels, rows, cols = field_ref.shape
    bands = table_ref.shape[2]
    me_x, me_y = lax.axis_index("gx"), lax.axis_index("gy")

    def peer_x(shift):
        return {"gx": lax.rem(me_x + n_gx - shift, n_gx)}

    def peer_y(shift):
        return {"gy": lax.rem(me_y + shift, n_gy)}

    barrier = pltpu.get_barrier_semaphore()
    for shift in range(1, n_gx):
        pl.semaphore_signal(barrier, inc=1, device_id=peer_x(shift), device_id_type=MESH)
    for shift in range(1, n_gy):
        pl.semaphore_signal(barrier, inc=1, device_id=peer_y(shift), device_id_type=MESH)
    pl.semaphore_wait(barrier, n_gx + n_gy - 2)

    def edge_x(shift):
        return pltpu.make_async_remote_copy(
            src_ref=edge_ref, dst_ref=xedge.at[shift - 1], send_sem=es.at[shift - 1],
            recv_sem=er.at[shift - 1], device_id=peer_x(shift), device_id_type=MESH)

    def rows_x(shift, level):
        return pltpu.make_async_remote_copy(
            src_ref=field_ref.at[level], dst_ref=xgot.at[shift - 1, level],
            send_sem=xs.at[shift - 1, level], recv_sem=xr.at[shift - 1, level],
            device_id=peer_x(shift), device_id_type=MESH)

    def edge_y(shift):
        return pltpu.make_async_remote_copy(
            src_ref=esend.at[shift - 1], dst_ref=out_edge_ref.at[shift], send_sem=ts.at[shift - 1],
            recv_sem=tr.at[shift - 1], device_id=peer_y(shift), device_id_type=MESH)

    def spec_y(shift, level):
        return pltpu.make_async_remote_copy(
            src_ref=send.at[shift - 1, level], dst_ref=out_ref.at[shift, level],
            send_sem=zs.at[shift - 1, level], recv_sem=zr.at[shift - 1, level],
            device_id=peer_y(shift), device_id_type=MESH)

    for shift in range(1, n_gx):
        edge_x(shift).start()

    @pl.loop(0, levels)
    def _(level):
        for shift in range(1, n_gx):
            rows_x(shift, level).start()

    tail = (cols - 1) // LANES * LANES

    def zone_of(parts):
        first = second = last = before = 0.0
        for at, part in enumerate(parts):
            owner = lax.rem(me_x + at, n_gx)
            is_first = jnp.where(owner == 0, 1.0, 0.0)
            is_last = jnp.where(owner == n_gx - 1, 1.0, 0.0)
            head = part[:, :min(LANES, cols)].astype(jnp.float32)
            rear = part[:, tail:].astype(jnp.float32)
            first += is_first * head[:, 0:1]
            second += is_first * head[:, 1:2]
            before += is_last * rear[:, cols - 2 - tail:cols - 1 - tail]
            last += is_last * rear[:, cols - 1 - tail:cols - tail]
        tangent = EXT_ZONE + 1.0
        zone = (last * weight_ref[0:1, :] + (tangent * (last - before)) * weight_ref[1:2, :]
                + first * weight_ref[2:3, :] + (tangent * (second - first)) * weight_ref[3:4, :])
        return zone.astype(jnp.bfloat16)

    def dot(a, b):
        return lax.dot_general(a, b, NT, preferred_element_type=jnp.float32)

    for shift in range(1, n_gx):
        edge_x(shift).wait_recv()
    parts = [edge_ref[...]] + [xedge[at] for at in range(n_gx - 1)]
    zone = zone_of(parts)
    for shift in range(n_gy):
        total = dot(zone, ztable_ref[shift])
        for at, part in enumerate(parts):
            total += dot(part, table_ref[at, shift])
        if shift == 0:
            out_edge_ref[0] = total
        else:
            esend[shift - 1] = total
            edge_y(shift).start()

    merged = bands % 16 == 0

    @pl.loop(0, levels)
    def _(level):
        for shift in range(1, n_gx):
            rows_x(shift, level).wait_recv()
        parts = [field_ref[level]] + [xgot[at, level] for at in range(n_gx - 1)]
        zone = zone_of(parts)
        if merged:
            size = n_gy * bands
            total = dot(ztable_ref[...].reshape(size, LANES), zone)
            for at, part in enumerate(parts):
                total += dot(table_ref[at].reshape(size, cols), part)
            pieces = [total[s * bands:(s + 1) * bands] for s in range(n_gy)]
        else:
            pieces = []
            for shift in range(n_gy):
                total = dot(ztable_ref[shift], zone)
                for at, part in enumerate(parts):
                    total += dot(table_ref[at, shift], part)
                pieces.append(total)
        for shift in range(n_gy):
            piece = pieces[shift].astype(jnp.bfloat16)
            if shift == 0:
                out_ref[0, level] = piece
            else:
                send[shift - 1, level] = piece
        for shift in range(1, n_gy):
            spec_y(shift, level).start()

    for shift in range(1, n_gx):
        edge_x(shift).wait_send()
    for shift in range(1, n_gy):
        edge_y(shift).wait()

    @pl.loop(0, levels)
    def _(level):
        for shift in range(1, n_gx):
            rows_x(shift, level).wait_send()
        for shift in range(1, n_gy):
            spec_y(shift, level).wait()


def make_plain_body(mesh):
    n_gx, n_gy = mesh.shape["gx"], mesh.shape["gy"]

    def body(field):
        levels, rows, cols = field.shape
        nx, ny = cols * n_gx, rows * n_gy
        length = nx + EXT_ZONE
        me_x, me_y = lax.axis_index("gx"), lax.axis_index("gy")
        bands = nx // (n_gx * n_gy)
        assert (nx // 2) % bands == 0
        group = 16 if bands % 16 == 0 else bands

        at = jnp.arange(nx + LANES, dtype=jnp.int32)
        column = jnp.where(at < nx, (at + me_x * cols) % nx, at)
        shift_at = jnp.arange(n_gy, dtype=jnp.int32)[:, None]
        coeff = ((me_y + shift_at) % n_gy) * (n_gx * bands) + me_x * bands
        coeff = (coeff + jnp.arange(0, bands, group, dtype=jnp.int32)[None, :]).reshape(-1)
        factors = wave_factors(coeff, group, column, nx // 2, length)
        p, q, c, s = lax.optimization_barrier(factors)

        def expand(lo, hi):
            full = p[:, None, lo:hi] * c[None, :, lo:hi] - q[:, None, lo:hi] * s[None, :, lo:hi]
            return full.astype(jnp.bfloat16).reshape(n_gy, bands, hi - lo)

        table = jnp.stack([expand(i * cols, (i + 1) * cols) for i in range(n_gx)])
        ztable = expand(nx, nx + LANES)
        ztable = jnp.where(jnp.arange(LANES) < EXT_ZONE, ztable, jnp.zeros_like(ztable))
        weights = jnp.pad(jnp.stack(blend_weights(EXT_ZONE)), ((0, 4), (0, LANES - EXT_ZONE)))
        edge = jnp.concatenate([field[:, :2], field[:, rows - 2:]], axis=1)
        edge = edge.transpose(1, 0, 2).reshape(4 * levels, cols)

        vmem = pl.BlockSpec(memory_space=pltpu.VMEM)
        dma = pltpu.SemaphoreType.DMA
        xs, ys = n_gx - 1, n_gy - 1
        got, edge_got = pl.pallas_call(
            functools.partial(kernel, n_gx, n_gy),
            out_shape=(
                jax.ShapeDtypeStruct((n_gy, levels, bands, rows), jnp.bfloat16),
                jax.ShapeDtypeStruct((n_gy, 4 * levels, bands), jnp.float32),
            ),
            in_specs=[vmem] * 5,
            out_specs=(vmem, vmem),
            scratch_shapes=[
                pltpu.VMEM((xs, levels, rows, cols), jnp.bfloat16),
                pltpu.VMEM((xs, 4 * levels, cols), jnp.bfloat16),
                pltpu.VMEM((ys, levels, bands, rows), jnp.bfloat16),
                pltpu.VMEM((ys, 4 * levels, bands), jnp.float32),
                dma((xs, levels)), dma((xs, levels)), dma((xs,)), dma((xs,)),
                dma((ys, levels)), dma((ys, levels)), dma((ys,)), dma((ys,)),
            ],
            compiler_params=pltpu.CompilerParams(collective_id=0, has_side_effects=True),
        )(field, edge, table, ztable, weights)

        edge_got = edge_got.reshape(n_gy, 4, levels, bands)
        low = lax.dynamic_index_in_dim(edge_got, me_y, 0, keepdims=False)
        high = lax.dynamic_index_in_dim(edge_got, (me_y + 1) % n_gy, 0, keepdims=False)
        low, high = low.transpose(0, 2, 1), high.transpose(0, 2, 1)
        spectra_zone = blend_zone(high[2], high[3], low[0], low[1], EXT_ZONE)

        spectra = jnp.zeros((bands, levels, ny), jnp.float32)
        for shift in range(n_gy):
            full = got[shift].transpose(1, 0, 2).astype(jnp.float32)
            source = (me_y + n_gy - shift) % n_gy
            spectra = lax.dynamic_update_slice(spectra, full, (0, 0, source * rows))
        return spectra, spectra_zone

    return body


ROWS = 128
GROUP = 16


def host_weights(zone_count):
    t = (np.arange(zone_count, dtype=np.float32) + np.float32(1)) / np.float32(zone_count + 1.0)
    two, three, one = np.float32(2), np.float32(3), np.float32(1)
    cube, square = t * t * t, t * t
    return (two * cube - three * square + one, cube - two * square + t,
            three * square - two * cube, cube - square)


def unit_circle(product, length):
    quarter = length / 4.0
    turns = jnp.floor(product * (4.0 / length) + 0.5)
    theta = (product - turns * quarter) * (2.0 * math.pi / length)
    turns = turns - 4.0 * jnp.floor(turns * 0.25)
    z = theta * theta
    sin = theta * (1.0 + z * (-1.0 / 6 + z * (1.0 / 120 + z * (-1.0 / 5040 + z * (1.0 / 362880)))))
    cos = 1.0 + z * (-0.5 + z * (1.0 / 24 + z * (-1.0 / 720 + z * (1.0 / 40320 - z * (1.0 / 3628800)))))
    odd = (turns == 1.0) | (turns == 3.0)
    c, s = jnp.where(odd, sin, cos), jnp.where(odd, cos, sin)
    c = jnp.where((turns == 1.0) | (turns == 2.0), -c, c)
    s = jnp.where(turns >= 2.0, -s, s)
    return c, s


def fused_kernel(n_gx, n_gy, field_ref, out_ref, zone_ref,
                 own, xgot, got, send, tab, ztab, zbuf, pq, cs, acc, esum, esend, egot,
                 ls, xs, xr, zs, zr, fs, fr, far, *, depth, lag):
    levels, rows, cols = field_ref.shape
    bands = got.shape[2]
    nblk, share = rows // ROWS, levels // n_gx
    half = n_gy // 2 * n_gx * bands
    nx = n_gx * cols
    length = nx + EXT_ZONE
    me_x, me_y = lax.axis_index("gx"), lax.axis_index("gy")
    chunks = share * nblk
    blocks = [(k, x) for k in range(n_gy - 1) for x in range(n_gx)]
    blocks += [(n_gy - 1, x) for x in range(1, n_gx)] + [(n_gy - 1, 0)]

    def peer_x(shift):
        return {"gx": lax.rem(me_x + n_gx - shift, n_gx)}

    def peer_y(shift):
        return {"gy": lax.rem(me_y + shift, n_gy)}

    def turn(k):
        up, down = n_gy - 1 - k, k
        if k == n_gy - 1:
            return 0
        up = jnp.where(up > me_y, up, up - 1)
        down = jnp.where(down < me_y, down, down + 1)
        return lax.rem(jnp.where(2 * me_y < n_gy, up, down) - me_y + n_gy, n_gy)

    above, below = me_y < n_gy - 1, me_y > 0

    def tell(semaphore, up):
        pl.semaphore_signal(semaphore, inc=1, device_id={"gy": me_y + (1 if up else -1)},
                            device_id_type=MESH)

    barrier = pltpu.get_barrier_semaphore()
    for shift in range(1, n_gx):
        pl.semaphore_signal(barrier, inc=1, device_id=peer_x(shift), device_id_type=MESH)
    pl.when(above)(lambda: tell(barrier, True))
    pl.when(below)(lambda: tell(barrier, False))

    def vouch():
        pl.when(above & below)(lambda: tell(far.at[0], False))
        pl.when(above & below)(lambda: tell(far.at[1], True))

    def hear():
        for hop in range(n_gy - 2):
            @pl.when(me_y + hop < n_gy - 2)
            def _():
                pl.semaphore_wait(far.at[0], 1)
                pl.when(below)(lambda: tell(far.at[0], False))

            @pl.when(me_y - hop > 1)
            def _():
                pl.semaphore_wait(far.at[1], 1)
                pl.when(above)(lambda: tell(far.at[1], True))

        for shift in range(1, n_gx):
            pl.semaphore_signal(far.at[2], inc=1, device_id=peer_x(shift), device_id_type=MESH)
        pl.semaphore_wait(far.at[2], n_gx - 1)

    def place(i, owner):
        ahead = jnp.where(owner == n_gy - 1, nblk - 1, 0)
        return lax.rem(i // share + ahead, nblk), lax.rem(i, share)

    def lines(blk):
        return pl.ds(pl.multiple_of(blk * ROWS, ROWS), ROWS)

    def load(turn_at):
        blk, _ = place(turn_at * share, me_y)
        at = lines(blk)
        return pltpu.make_async_copy(
            field_ref.at[pl.ds(me_x * share, share), at], own.at[:, at], ls.at[turn_at])

    def rows_x(shift, i):
        blk, level = place(i, me_y)
        at = lines(blk)
        peer = peer_x(shift)
        return pltpu.make_async_remote_copy(
            src_ref=field_ref.at[peer["gx"] * share + level, at], dst_ref=xgot.at[shift - 1, level, at],
            send_sem=xs.at[shift - 1], recv_sem=xr.at[i], device_id=peer, device_id_type=MESH)

    def rows_in(i):
        blk, level = place(i, me_y)
        ref = xgot.at[:, level, lines(blk)]
        return pltpu.make_async_remote_copy(
            src_ref=ref, dst_ref=ref, send_sem=xs.at[0], recv_sem=xr.at[i],
            device_id=peer_x(1), device_id_type=MESH)

    def owner_of(b):
        k, x = blocks[b]
        return {"gy": lax.rem(me_y + turn(k), n_gy), "gx": lax.rem(me_x + x, n_gx)}

    def spec(b, i):
        return pltpu.make_async_remote_copy(
            src_ref=send.at[b, i], dst_ref=got.at[me_y * n_gx + me_x, i],
            send_sem=zs, recv_sem=zr.at[i], device_id=owner_of(b), device_id_type=MESH)

    def specs_in(i):
        return pltpu.make_async_remote_copy(
            src_ref=send.at[:, 0], dst_ref=got.at[pl.ds(0, len(blocks) - 1), 0],
            send_sem=zs, recv_sem=zr.at[i], device_id=peer_y(1), device_id_type=MESH)

    def edge(side, b):
        return pltpu.make_async_remote_copy(
            src_ref=esend.at[b], dst_ref=egot.at[side, me_x], send_sem=fs, recv_sem=fr.at[side, me_x],
            device_id=owner_of(b), device_id_type=MESH)

    def edge_in(side, x):
        return pltpu.make_async_remote_copy(
            src_ref=esend.at[0], dst_ref=egot.at[side, x], send_sem=fs, recv_sem=fr.at[side, x],
            device_id=peer_y(1), device_id_type=MESH)

    def all_sent(ref, semaphore):
        pltpu.make_async_remote_copy(
            src_ref=ref, dst_ref=ref, send_sem=semaphore, recv_sem=fr.at[0, 0],
            device_id=peer_y(1), device_id_type=MESH).wait_send()

    for turn_at in range(nblk):
        load(turn_at).start()

    pl.semaphore_wait(barrier, n_gx - 1 + above.astype(jnp.int32) + below.astype(jnp.int32))

    def send_ahead():
        @pl.loop(0, depth)
        def _(i):
            for shift in range(1, n_gx):
                rows_x(shift, i).start()

    leads = lax.axis_index("lev") != 0
    pl.when(leads)(send_ahead)
    vouch()

    norm = 1.0 / math.sqrt(length)
    ngroup = half // GROUP
    lane = lax.broadcasted_iota(jnp.int32, (1, LANES), 1)

    def build(part):
        row0 = part * half
        g = lax.broadcasted_iota(jnp.int32, (ngroup, 1), 0) * GROUP + row0
        block = g // bands
        origin = jnp.zeros((ngroup, 1), jnp.int32)
        for b in range(row0 // bands, (row0 + half) // bands):
            to = owner_of(b)
            origin = jnp.where(block == b, (to["gy"] * n_gx + to["gx"]) * bands, origin)
        first = origin + (g - block * bands)
        is_cos = first < nx // 2
        number = jnp.where(is_cos, first, first - (nx // 2 - 1)).astype(jnp.float32)
        step = lax.broadcasted_iota(jnp.int32, (GROUP, 1), 0).astype(jnp.float32)

        def factors(column, width):
            c, s = unit_circle(number * column, length)
            pq[0, :, :width], pq[1, :, :width] = jnp.where(is_cos, c, -s), jnp.where(is_cos, s, c)
            c, s = unit_circle(step * column, length)
            cs[0, :, :width], cs[1, :, :width] = c * norm, s * norm

        def expand(write, width):
            @pl.loop(0, ngroup // 8)
            def _(k):
                at = pl.ds(pl.multiple_of(k * 8, 8), 8)
                for r in range(8):
                    p, q = pq[0, at, :width][r:r + 1], pq[1, at, :width][r:r + 1]
                    write(pl.ds(pl.multiple_of(row0 + (k * 8 + r) * GROUP, GROUP), GROUP),
                          p * cs[0, :, :width] - q * cs[1, :, :width])

        for at in range(n_gx):
            base = (lax.rem(me_x + at, n_gx) * cols).astype(jnp.float32)
            factors(lax.broadcasted_iota(jnp.int32, (1, cols), 1).astype(jnp.float32) + base, cols)

            def write(to, value, at=at):
                tab[at, to, :] = value.astype(jnp.bfloat16)

            expand(write, cols)
            if part == 0 and at == 0:
                pl.when(jnp.logical_not(leads))(send_ahead)
        factors(lane.astype(jnp.float32) + float(nx), LANES)

        def write_zone(to, value):
            ztab[to, :] = jnp.where(lane < EXT_ZONE, value, 0.0).astype(jnp.bfloat16)

        expand(write_zone, LANES)

    t = jnp.minimum(lane + 1, EXT_ZONE).astype(jnp.float32) / (EXT_ZONE + 1.0)
    cube, square = t * t * t, t * t
    weight_a = 2.0 * cube - 3.0 * square + 1.0
    weight_b = cube - 2.0 * square + t
    weight_c = -2.0 * cube + 3.0 * square
    weight_d = cube - square
    tangent = EXT_ZONE + 1.0
    tail = cols - LANES

    def zone_of(parts):
        first = second = last = before = 0.0
        for at, part in enumerate(parts):
            owner = lax.rem(me_x + at, n_gx)
            is_first = jnp.where(owner == 0, 1.0, 0.0)
            is_last = jnp.where(owner == n_gx - 1, 1.0, 0.0)
            head = part[:, :LANES].astype(jnp.float32)
            rear = part[:, tail:].astype(jnp.float32)
            first += is_first * head[:, 0:1]
            second += is_first * head[:, 1:2]
            before += is_last * rear[:, LANES - 2:LANES - 1]
            last += is_last * rear[:, LANES - 1:LANES]
        zone = (last * weight_a + (tangent * (last - before)) * weight_b
                + first * weight_c + (tangent * (second - first)) * weight_d)
        return zone.astype(jnp.bfloat16)

    def dot(a, b):
        return lax.dot_general(a, b, NT, preferred_element_type=jnp.float32)

    def arrive(i):
        specs_in(i).wait_recv()
        for source in range(n_gy * n_gx):
            blk, level = place(i, source // n_gx)
            level += source % n_gx * share
            out_ref[source // n_gx * nblk + blk, pl.ds(level, bands, stride=levels), :] = (
                got[source, i].astype(jnp.float32))

    def own_part(i, part):
        blk, level = place(i, me_y)
        at = pl.ds(part * half, half)
        acc[at, :] = dot(tab[0, at, :], own[level, lines(blk), :])

    def blend(i):
        blk, level = place(i, me_y)
        at = lines(blk)
        zbuf[...] = zone_of([own[level, at, :]] + [xgot[x, level, at, :] for x in range(n_gx - 1)])

    def finish(i, lo, hi):
        blk, level = place(i, me_y)
        at = pl.ds(lo * bands, (hi - lo) * bands)
        total = acc[at, :] + dot(ztab[at, :], zbuf[...])
        for x in range(1, n_gx):
            total += dot(tab[x, at, :], xgot[x - 1, level, lines(blk), :])
        for b in range(lo, hi):
            piece = total[(b - lo) * bands:(b - lo + 1) * bands].astype(jnp.bfloat16)
            if b == len(blocks) - 1:
                got[me_y * n_gx + me_x, i] = piece
            else:
                send[b, i] = piece
                spec(b, i).start()

    def far_pieces(i):
        for lo in range(0, half // bands, n_gx):
            finish(i, lo, lo + n_gx)

    def near_pieces(i):
        finish(i, half // bands, len(blocks))

    def edges():
        top = me_y == 0
        row0 = pl.multiple_of(jnp.where(top, 0, rows - 16), 16)
        parts = [own[:, pl.ds(row0, 16), :].reshape(share * 16, cols)]
        parts += [xgot[x, :, pl.ds(row0, 16), :].reshape(share * 16, cols) for x in range(n_gx - 1)]
        total = dot(zone_of(parts), ztab[...])
        for x, part in enumerate(parts):
            total += dot(part, tab[x])
        esum[...] = total
        for pair in range(2):
            for level in range(share):
                upper = esum[level * 16 + pair:level * 16 + pair + 1, :]
                lower = esum[level * 16 + 14 + pair:level * 16 + 15 + pair, :]
                line = jnp.where(top, upper, lower)
                row = pair * share + level
                for b in range(len(blocks)):
                    esend[b, row:row + 1, :] = line[:, b * bands:(b + 1) * bands]
        for side, owner in ((0, 0), (1, n_gy - 1)):
            @pl.when(me_y == owner)
            def _(side=side):
                egot[side, me_x] = esend[len(blocks) - 1]
                for b in range(len(blocks) - 1):
                    edge(side, b).start()

    seam = (me_y == 0) | (me_y == n_gy - 1)

    def rows_ready(i):
        rows_in(i).wait_recv()

        @pl.when(i + depth < chunks)
        def _():
            for shift in range(1, n_gx):
                rows_x(shift, i + depth).start()

        blend(i)

    build(0)
    load(0).wait()
    own_part(0, 0)
    hear()
    rows_ready(0)
    far_pieces(0)
    build(1)
    own_part(0, 1)
    near_pieces(0)

    @pl.loop(1, chunks)
    def _(i):
        for turn_at in range(1, nblk):
            @pl.when(i == turn_at * share)
            def _():
                load(turn_at).wait()

        own_part(i, 0)
        own_part(i, 1)
        rows_ready(i)
        far_pieces(i)
        near_pieces(i)

        @pl.when(seam & (i == share - 1))
        def _():
            edges()

        @pl.when(i >= lag)
        def _():
            arrive(i - lag)

    for side, owner in ((0, 0), (1, n_gy - 1)):
        for x in range(n_gx):
            @pl.when((me_y != owner) | (me_x != x))
            def _(side=side, x=x):
                edge_in(side, x).wait_recv()

    pl.when(seam)(lambda: all_sent(esend.at[pl.ds(0, len(blocks) - 1)], fs))
    wa, wb, wc, wd = host_weights(EXT_ZONE)
    for x in range(n_gx):
        first, second = egot[0, x, :share, :], egot[0, x, share:, :]
        before, last = egot[1, x, :share, :], egot[1, x, share:, :]
        slope_start, slope_end = tangent * (last - before), tangent * (second - first)
        for j in range(EXT_ZONE):
            zone_ref[j, x * share:(x + 1) * share, :] = (
                last * float(wa[j]) + slope_start * float(wb[j])
                + first * float(wc[j]) + slope_end * float(wd[j]))

    for shift in range(1, n_gx):
        all_sent(field_ref.at[pl.ds(0, share)], xs.at[shift - 1])

    @pl.loop(chunks - lag, chunks)
    def _(i):
        arrive(i)

    all_sent(send, zs)


def make_fused_body(mesh):
    n_gx, n_gy = mesh.shape["gx"], mesh.shape["gy"]

    def body(field):
        levels, rows, cols = field.shape
        bands = cols // n_gy
        nblk, ny, size = rows // ROWS, rows * n_gy, n_gy * n_gx * bands
        share, xs, peers = levels // n_gx, n_gx - 1, n_gy * n_gx - 1
        chunks = share * nblk
        vmem, dma = pl.BlockSpec(memory_space=pltpu.VMEM), pltpu.SemaphoreType.DMA
        bf16, f32 = jnp.bfloat16, jnp.float32
        spectra, zone = pl.pallas_call(
            functools.partial(fused_kernel, n_gx, n_gy, depth=DEPTH, lag=LAG),
            out_shape=(
                jax.ShapeDtypeStruct((n_gy * nblk, bands * levels, ROWS), f32),
                jax.ShapeDtypeStruct((EXT_ZONE, levels, bands), f32),
            ),
            in_specs=[pl.BlockSpec(memory_space=pltpu.HBM)],
            out_specs=(vmem, vmem),
            scratch_shapes=[
                pltpu.VMEM((share, rows, cols), bf16),
                pltpu.VMEM((xs, share, rows, cols), bf16),
                pltpu.VMEM((peers + 1, chunks, bands, ROWS), bf16),
                pltpu.VMEM((peers, chunks, bands, ROWS), bf16),
                pltpu.VMEM((n_gx, size, cols), bf16),
                pltpu.VMEM((size, LANES), bf16),
                pltpu.VMEM((ROWS, LANES), bf16),
                pltpu.VMEM((2, size // 2 // GROUP, cols), f32),
                pltpu.VMEM((2, GROUP, cols), f32),
                pltpu.VMEM((size, ROWS), f32),
                pltpu.VMEM((share * 16, size), f32),
                pltpu.VMEM((peers + 1, 2 * share, bands), f32),
                pltpu.VMEM((2, n_gx, 2 * share, bands), f32),
                dma((nblk,)), dma((xs,)), dma((chunks,)), dma, dma((chunks,)),
                dma, dma((2, n_gx)), pltpu.SemaphoreType.REGULAR((3,)),
            ],
            compiler_params=pltpu.CompilerParams(
                collective_id=0, has_side_effects=True, vmem_limit_bytes=VMEM_LIMIT),
        )(pltpu.with_memory_space_constraint(field, pltpu.HBM))
        spectra, zone = pl.pallas_call(
            store_kernel,
            out_shape=(
                jax.ShapeDtypeStruct((bands * levels, ny), f32),
                jax.ShapeDtypeStruct(zone.shape, f32),
            ),
            in_specs=[vmem, vmem],
            out_specs=(pl.BlockSpec(memory_space=pl.ANY),) * 2,
            scratch_shapes=[dma((n_gy * nblk + 1,))],
            compiler_params=pltpu.CompilerParams(vmem_limit_bytes=VMEM_LIMIT_STORE),
        )(spectra, zone)
        return spectra.reshape(bands, levels, ny), zone.transpose(2, 1, 0)

    return body


def store_kernel(tile_ref, zone_ref, out_ref, zone_out_ref, sem):
    count = tile_ref.shape[0]
    copies = [
        pltpu.make_async_copy(tile_ref.at[b], out_ref.at[:, pl.ds(b * ROWS, ROWS)], sem.at[b])
        for b in range(count)
    ]
    copies.append(pltpu.make_async_copy(zone_ref, zone_out_ref, sem.at[count]))
    for copy in copies:
        copy.start()
    for copy in copies:
        copy.wait()


VMEM_LIMIT_STORE = 16 * 2**20
DEPTH = 3
LAG = 3
VMEM_LIMIT = 36 * 2**20


def fits(mesh, shape):
    n_gx, n_gy = mesh.shape["gx"], mesh.shape["gy"]
    levels = shape[0] // (mesh.shape["member"] * mesh.shape["lev"])
    rows, cols = shape[1] // n_gy, shape[2] // n_gx
    bands = cols // n_gy
    return (n_gx > 1 and n_gy > 1 and n_gy % 2 == 0 and rows % ROWS == 0 and cols % LANES == 0
            and bands % GROUP == 0 and n_gy * n_gx * bands % (16 * GROUP) == 0
            and (cols * n_gx // 2) % bands == 0 and levels % 8 == 0 and levels % (2 * n_gx) == 0
            and levels // n_gx * rows // ROWS > max(DEPTH, LAG))


def solution(mesh):
    def program(field):
        body = make_fused_body(mesh) if fits(mesh, field.shape) else make_plain_body(mesh)
        return jax.shard_map(
            body,
            mesh=mesh,
            in_specs=(P(("member", "lev"), "gy", "gx"),),
            out_specs=(
                P(("gy", "gx"), ("member", "lev"), None),
                P(("gy", "gx"), ("member", "lev"), None),
            ),
            check_vma=False,
        )(field)

    return program
```

```python
import functools
import math

import jax
import jax.numpy as jnp
import numpy as np
from jax import lax
from jax.experimental import pallas as pl
from jax.experimental.pallas import tpu as pltpu
from jax.sharding import PartitionSpec as P

EXT_ZONE = 11
LANES = 128
NT = (((1,), (1,)), ((), ()))
MESH = pl.DeviceIdType.MESH


def blend_weights(zone_count):
    steps = (jnp.arange(zone_count, dtype=jnp.int32) + 1).astype(jnp.float32) / (zone_count + 1.0)
    weight_a = 2.0 * steps**3 - 3.0 * steps**2 + 1.0
    weight_b = steps**3 - 2.0 * steps**2 + steps
    weight_c = -2.0 * steps**3 + 3.0 * steps**2
    weight_d = steps**3 - steps**2
    return weight_a, weight_b, weight_c, weight_d


def blend_zone(second_last, last_value, first_value, second_value, zone_count):
    weight_a, weight_b, weight_c, weight_d = blend_weights(zone_count)
    tangent_scale = zone_count + 1.0
    slope_start = tangent_scale * (last_value - second_last)
    slope_end = tangent_scale * (second_value - first_value)
    return (
        last_value[..., None] * weight_a
        + slope_start[..., None] * weight_b
        + first_value[..., None] * weight_c
        + slope_end[..., None] * weight_d
    )


def wave_factors(coeff0, group, column, wave_count, length):
    number0 = jnp.where(coeff0 < wave_count, coeff0, coeff0 - wave_count + 1)
    scale = 2.0 * math.pi / length
    phase0 = (number0[:, None] * column[None, :] % length).astype(jnp.float32) * scale
    cos0, sin0 = jnp.cos(phase0), jnp.sin(phase0)
    is_cosine = (coeff0 < wave_count)[:, None]
    p, q = jnp.where(is_cosine, cos0, -sin0), jnp.where(is_cosine, sin0, cos0)
    step = jnp.arange(group, dtype=jnp.int32)
    phase = (step[:, None] * column[None, :] % length).astype(jnp.float32) * scale
    norm = 1.0 / math.sqrt(length)
    return p, q, jnp.cos(phase) * norm, jnp.sin(phase) * norm


def kernel(n_gx, n_gy, field_ref, edge_ref, table_ref, ztable_ref, weight_ref,
           out_ref, out_edge_ref, xgot, xedge, send, esend, xs, xr, es, er, zs, zr, ts, tr):
    levels, rows, cols = field_ref.shape
    bands = table_ref.shape[2]
    me_x, me_y = lax.axis_index("gx"), lax.axis_index("gy")

    def peer_x(shift):
        return {"gx": lax.rem(me_x + n_gx - shift, n_gx)}

    def peer_y(shift):
        return {"gy": lax.rem(me_y + shift, n_gy)}

    barrier = pltpu.get_barrier_semaphore()
    for shift in range(1, n_gx):
        pl.semaphore_signal(barrier, inc=1, device_id=peer_x(shift), device_id_type=MESH)
    for shift in range(1, n_gy):
        pl.semaphore_signal(barrier, inc=1, device_id=peer_y(shift), device_id_type=MESH)
    pl.semaphore_wait(barrier, n_gx + n_gy - 2)

    def edge_x(shift):
        return pltpu.make_async_remote_copy(
            src_ref=edge_ref, dst_ref=xedge.at[shift - 1], send_sem=es.at[shift - 1],
            recv_sem=er.at[shift - 1], device_id=peer_x(shift), device_id_type=MESH)

    def rows_x(shift, level):
        return pltpu.make_async_remote_copy(
            src_ref=field_ref.at[level], dst_ref=xgot.at[shift - 1, level],
            send_sem=xs.at[shift - 1, level], recv_sem=xr.at[shift - 1, level],
            device_id=peer_x(shift), device_id_type=MESH)

    def edge_y(shift):
        return pltpu.make_async_remote_copy(
            src_ref=esend.at[shift - 1], dst_ref=out_edge_ref.at[shift], send_sem=ts.at[shift - 1],
            recv_sem=tr.at[shift - 1], device_id=peer_y(shift), device_id_type=MESH)

    def spec_y(shift, level):
        return pltpu.make_async_remote_copy(
            src_ref=send.at[shift - 1, level], dst_ref=out_ref.at[shift, level],
            send_sem=zs.at[shift - 1, level], recv_sem=zr.at[shift - 1, level],
            device_id=peer_y(shift), device_id_type=MESH)

    for shift in range(1, n_gx):
        edge_x(shift).start()

    @pl.loop(0, levels)
    def _(level):
        for shift in range(1, n_gx):
            rows_x(shift, level).start()

    tail = (cols - 1) // LANES * LANES

    def zone_of(parts):
        first = second = last = before = 0.0
        for at, part in enumerate(parts):
            owner = lax.rem(me_x + at, n_gx)
            is_first = jnp.where(owner == 0, 1.0, 0.0)
            is_last = jnp.where(owner == n_gx - 1, 1.0, 0.0)
            head = part[:, :min(LANES, cols)].astype(jnp.float32)
            rear = part[:, tail:].astype(jnp.float32)
            first += is_first * head[:, 0:1]
            second += is_first * head[:, 1:2]
            before += is_last * rear[:, cols - 2 - tail:cols - 1 - tail]
            last += is_last * rear[:, cols - 1 - tail:cols - tail]
        tangent = EXT_ZONE + 1.0
        zone = (last * weight_ref[0:1, :] + (tangent * (last - before)) * weight_ref[1:2, :]
                + first * weight_ref[2:3, :] + (tangent * (second - first)) * weight_ref[3:4, :])
        return zone.astype(jnp.bfloat16)

    def dot(a, b):
        return lax.dot_general(a, b, NT, preferred_element_type=jnp.float32)

    for shift in range(1, n_gx):
        edge_x(shift).wait_recv()
    parts = [edge_ref[...]] + [xedge[at] for at in range(n_gx - 1)]
    zone = zone_of(parts)
    for shift in range(n_gy):
        total = dot(zone, ztable_ref[shift])
        for at, part in enumerate(parts):
            total += dot(part, table_ref[at, shift])
        if shift == 0:
            out_edge_ref[0] = total
        else:
            esend[shift - 1] = total
            edge_y(shift).start()

    merged = bands % 16 == 0

    @pl.loop(0, levels)
    def _(level):
        for shift in range(1, n_gx):
            rows_x(shift, level).wait_recv()
        parts = [field_ref[level]] + [xgot[at, level] for at in range(n_gx - 1)]
        zone = zone_of(parts)
        if merged:
            size = n_gy * bands
            total = dot(ztable_ref[...].reshape(size, LANES), zone)
            for at, part in enumerate(parts):
                total += dot(table_ref[at].reshape(size, cols), part)
            pieces = [total[s * bands:(s + 1) * bands] for s in range(n_gy)]
        else:
            pieces = []
            for shift in range(n_gy):
                total = dot(ztable_ref[shift], zone)
                for at, part in enumerate(parts):
                    total += dot(table_ref[at, shift], part)
                pieces.append(total)
        for shift in range(n_gy):
            piece = pieces[shift].astype(jnp.bfloat16)
            if shift == 0:
                out_ref[0, level] = piece
            else:
                send[shift - 1, level] = piece
        for shift in range(1, n_gy):
            spec_y(shift, level).start()

    for shift in range(1, n_gx):
        edge_x(shift).wait_send()
    for shift in range(1, n_gy):
        edge_y(shift).wait()

    @pl.loop(0, levels)
    def _(level):
        for shift in range(1, n_gx):
            rows_x(shift, level).wait_send()
        for shift in range(1, n_gy):
            spec_y(shift, level).wait()


def make_plain_body(mesh):
    n_gx, n_gy = mesh.shape["gx"], mesh.shape["gy"]

    def body(field):
        levels, rows, cols = field.shape
        nx, ny = cols * n_gx, rows * n_gy
        length = nx + EXT_ZONE
        me_x, me_y = lax.axis_index("gx"), lax.axis_index("gy")
        bands = nx // (n_gx * n_gy)
        assert (nx // 2) % bands == 0
        group = 16 if bands % 16 == 0 else bands

        at = jnp.arange(nx + LANES, dtype=jnp.int32)
        column = jnp.where(at < nx, (at + me_x * cols) % nx, at)
        shift_at = jnp.arange(n_gy, dtype=jnp.int32)[:, None]
        coeff = ((me_y + shift_at) % n_gy) * (n_gx * bands) + me_x * bands
        coeff = (coeff + jnp.arange(0, bands, group, dtype=jnp.int32)[None, :]).reshape(-1)
        factors = wave_factors(coeff, group, column, nx // 2, length)
        p, q, c, s = lax.optimization_barrier(factors)

        def expand(lo, hi):
            full = p[:, None, lo:hi] * c[None, :, lo:hi] - q[:, None, lo:hi] * s[None, :, lo:hi]
            return full.astype(jnp.bfloat16).reshape(n_gy, bands, hi - lo)

        table = jnp.stack([expand(i * cols, (i + 1) * cols) for i in range(n_gx)])
        ztable = expand(nx, nx + LANES)
        ztable = jnp.where(jnp.arange(LANES) < EXT_ZONE, ztable, jnp.zeros_like(ztable))
        weights = jnp.pad(jnp.stack(blend_weights(EXT_ZONE)), ((0, 4), (0, LANES - EXT_ZONE)))
        edge = jnp.concatenate([field[:, :2], field[:, rows - 2:]], axis=1)
        edge = edge.transpose(1, 0, 2).reshape(4 * levels, cols)

        vmem = pl.BlockSpec(memory_space=pltpu.VMEM)
        dma = pltpu.SemaphoreType.DMA
        xs, ys = n_gx - 1, n_gy - 1
        got, edge_got = pl.pallas_call(
            functools.partial(kernel, n_gx, n_gy),
            out_shape=(
                jax.ShapeDtypeStruct((n_gy, levels, bands, rows), jnp.bfloat16),
                jax.ShapeDtypeStruct((n_gy, 4 * levels, bands), jnp.float32),
            ),
            in_specs=[vmem] * 5,
            out_specs=(vmem, vmem),
            scratch_shapes=[
                pltpu.VMEM((xs, levels, rows, cols), jnp.bfloat16),
                pltpu.VMEM((xs, 4 * levels, cols), jnp.bfloat16),
                pltpu.VMEM((ys, levels, bands, rows), jnp.bfloat16),
                pltpu.VMEM((ys, 4 * levels, bands), jnp.float32),
                dma((xs, levels)), dma((xs, levels)), dma((xs,)), dma((xs,)),
                dma((ys, levels)), dma((ys, levels)), dma((ys,)), dma((ys,)),
            ],
            compiler_params=pltpu.CompilerParams(collective_id=0, has_side_effects=True),
        )(field, edge, table, ztable, weights)

        edge_got = edge_got.reshape(n_gy, 4, levels, bands)
        low = lax.dynamic_index_in_dim(edge_got, me_y, 0, keepdims=False)
        high = lax.dynamic_index_in_dim(edge_got, (me_y + 1) % n_gy, 0, keepdims=False)
        low, high = low.transpose(0, 2, 1), high.transpose(0, 2, 1)
        spectra_zone = blend_zone(high[2], high[3], low[0], low[1], EXT_ZONE)

        spectra = jnp.zeros((bands, levels, ny), jnp.float32)
        for shift in range(n_gy):
            full = got[shift].transpose(1, 0, 2).astype(jnp.float32)
            source = (me_y + n_gy - shift) % n_gy
            spectra = lax.dynamic_update_slice(spectra, full, (0, 0, source * rows))
        return spectra, spectra_zone

    return body


ROWS = 128
GROUP = 16


def host_weights(zone_count):
    t = (np.arange(zone_count, dtype=np.float32) + np.float32(1)) / np.float32(zone_count + 1.0)
    two, three, one = np.float32(2), np.float32(3), np.float32(1)
    cube, square = t * t * t, t * t
    return (two * cube - three * square + one, cube - two * square + t,
            three * square - two * cube, cube - square)


def unit_circle(product, length):
    quarter = length / 4.0
    turns = jnp.floor(product * (4.0 / length) + 0.5)
    theta = (product - turns * quarter) * (2.0 * math.pi / length)
    turns = turns - 4.0 * jnp.floor(turns * 0.25)
    z = theta * theta
    sin = theta * (1.0 + z * (-1.0 / 6 + z * (1.0 / 120 + z * (-1.0 / 5040 + z * (1.0 / 362880)))))
    cos = 1.0 + z * (-0.5 + z * (1.0 / 24 + z * (-1.0 / 720 + z * (1.0 / 40320 - z * (1.0 / 3628800)))))
    odd = (turns == 1.0) | (turns == 3.0)
    c, s = jnp.where(odd, sin, cos), jnp.where(odd, cos, sin)
    c = jnp.where((turns == 1.0) | (turns == 2.0), -c, c)
    s = jnp.where(turns >= 2.0, -s, s)
    return c, s


def fused_kernel(n_gx, n_gy, field_ref, out_ref, zone_ref,
                 own, xgot, got, send, tab, ztab, zbuf, pq, cs, acc, esum, esend, egot,
                 ls, xs, xr, zs, zr, fs, fr, far, *, depth, lags):
    levels, rows, cols = field_ref.shape
    bands = got.shape[2]
    nblk, share = rows // ROWS, levels // n_gx
    half = n_gy // 2 * n_gx * bands
    nx = n_gx * cols
    length = nx + EXT_ZONE
    me_x, me_y = lax.axis_index("gx"), lax.axis_index("gy")
    chunks = share * nblk
    blocks = [(k, x) for k in range(n_gy - 1) for x in range(n_gx)]
    blocks += [(n_gy - 1, x) for x in range(1, n_gx)] + [(n_gy - 1, 0)]

    def peer_x(shift):
        return {"gx": lax.rem(me_x + n_gx - shift, n_gx)}

    def peer_y(shift):
        return {"gy": lax.rem(me_y + shift, n_gy)}

    def turn(k):
        up, down = n_gy - 1 - k, k
        if k == n_gy - 1:
            return 0
        up = jnp.where(up > me_y, up, up - 1)
        down = jnp.where(down < me_y, down, down + 1)
        return lax.rem(jnp.where(2 * me_y < n_gy, up, down) - me_y + n_gy, n_gy)

    above, below = me_y < n_gy - 1, me_y > 0

    def tell(semaphore, up):
        pl.semaphore_signal(semaphore, inc=1, device_id={"gy": me_y + (1 if up else -1)},
                            device_id_type=MESH)

    barrier = pltpu.get_barrier_semaphore()
    for shift in range(1, n_gx):
        pl.semaphore_signal(barrier, inc=1, device_id=peer_x(shift), device_id_type=MESH)
    pl.when(above)(lambda: tell(barrier, True))
    pl.when(below)(lambda: tell(barrier, False))

    def vouch():
        pl.when(above & below)(lambda: tell(far.at[0], False))
        pl.when(above & below)(lambda: tell(far.at[1], True))

    def hear():
        for hop in range(n_gy - 2):
            @pl.when(me_y + hop < n_gy - 2)
            def _():
                pl.semaphore_wait(far.at[0], 1)
                pl.when(below)(lambda: tell(far.at[0], False))

            @pl.when(me_y - hop > 1)
            def _():
                pl.semaphore_wait(far.at[1], 1)
                pl.when(above)(lambda: tell(far.at[1], True))

        for shift in range(1, n_gx):
            pl.semaphore_signal(far.at[2], inc=1, device_id=peer_x(shift), device_id_type=MESH)
        pl.semaphore_wait(far.at[2], n_gx - 1)

    def place(i, owner):
        ahead = jnp.where(owner == n_gy - 1, nblk - 1, 0)
        return lax.rem(i // share + ahead, nblk), lax.rem(i, share)

    def lines(blk):
        return pl.ds(pl.multiple_of(blk * ROWS, ROWS), ROWS)

    def load(turn_at):
        blk, _ = place(turn_at * share, me_y)
        at = lines(blk)
        return pltpu.make_async_copy(
            field_ref.at[pl.ds(me_x * share, share), at], own.at[:, at], ls.at[turn_at])

    def rows_x(shift, i):
        blk, level = place(i, me_y)
        at = lines(blk)
        peer = peer_x(shift)
        return pltpu.make_async_remote_copy(
            src_ref=field_ref.at[peer["gx"] * share + level, at], dst_ref=xgot.at[shift - 1, level, at],
            send_sem=xs.at[shift - 1], recv_sem=xr.at[i], device_id=peer, device_id_type=MESH)

    def rows_in(i):
        blk, level = place(i, me_y)
        ref = xgot.at[:, level, lines(blk)]
        return pltpu.make_async_remote_copy(
            src_ref=ref, dst_ref=ref, send_sem=xs.at[0], recv_sem=xr.at[i],
            device_id=peer_x(1), device_id_type=MESH)

    def owner_of(b):
        k, x = blocks[b]
        return {"gy": lax.rem(me_y + turn(k), n_gy), "gx": lax.rem(me_x + x, n_gx)}

    def spec(b, i):
        return pltpu.make_async_remote_copy(
            src_ref=send.at[b, i], dst_ref=got.at[me_y * n_gx + me_x, i],
            send_sem=zs, recv_sem=zr.at[i], device_id=owner_of(b), device_id_type=MESH)

    def specs_in(i):
        return pltpu.make_async_remote_copy(
            src_ref=send.at[:, 0], dst_ref=got.at[pl.ds(0, len(blocks) - 1), 0],
            send_sem=zs, recv_sem=zr.at[i], device_id=peer_y(1), device_id_type=MESH)

    def edge(side, b):
        return pltpu.make_async_remote_copy(
            src_ref=esend.at[b], dst_ref=egot.at[side, me_x], send_sem=fs, recv_sem=fr.at[side, me_x],
            device_id=owner_of(b), device_id_type=MESH)

    def edge_in(side, x):
        return pltpu.make_async_remote_copy(
            src_ref=esend.at[0], dst_ref=egot.at[side, x], send_sem=fs, recv_sem=fr.at[side, x],
            device_id=peer_y(1), device_id_type=MESH)

    def all_sent(ref, semaphore):
        pltpu.make_async_remote_copy(
            src_ref=ref, dst_ref=ref, send_sem=semaphore, recv_sem=fr.at[0, 0],
            device_id=peer_y(1), device_id_type=MESH).wait_send()

    for turn_at in range(nblk):
        load(turn_at).start()

    pl.semaphore_wait(barrier, n_gx - 1 + above.astype(jnp.int32) + below.astype(jnp.int32))

    def send_ahead():
        @pl.loop(0, depth)
        def _(i):
            for shift in range(1, n_gx):
                rows_x(shift, i).start()

    leads = lax.axis_index("lev") != 0
    lag = jnp.where(leads, *lags)
    pl.when(leads)(send_ahead)
    vouch()

    norm = 1.0 / math.sqrt(length)
    ngroup = half // GROUP
    lane = lax.broadcasted_iota(jnp.int32, (1, LANES), 1)

    def build(part):
        row0 = part * half
        g = lax.broadcasted_iota(jnp.int32, (ngroup, 1), 0) * GROUP + row0
        block = g // bands
        origin = jnp.zeros((ngroup, 1), jnp.int32)
        for b in range(row0 // bands, (row0 + half) // bands):
            to = owner_of(b)
            origin = jnp.where(block == b, (to["gy"] * n_gx + to["gx"]) * bands, origin)
        first = origin + (g - block * bands)
        is_cos = first < nx // 2
        number = jnp.where(is_cos, first, first - (nx // 2 - 1)).astype(jnp.float32)
        step = lax.broadcasted_iota(jnp.int32, (GROUP, 1), 0).astype(jnp.float32)

        def factors(column, width):
            c, s = unit_circle(number * column, length)
            pq[0, :, :width], pq[1, :, :width] = jnp.where(is_cos, c, -s), jnp.where(is_cos, s, c)
            c, s = unit_circle(step * column, length)
            cs[0, :, :width], cs[1, :, :width] = c * norm, s * norm

        def expand(write, width):
            @pl.loop(0, ngroup // 8)
            def _(k):
                at = pl.ds(pl.multiple_of(k * 8, 8), 8)
                for r in range(8):
                    p, q = pq[0, at, :width][r:r + 1], pq[1, at, :width][r:r + 1]
                    write(pl.ds(pl.multiple_of(row0 + (k * 8 + r) * GROUP, GROUP), GROUP),
                          p * cs[0, :, :width] - q * cs[1, :, :width])

        for at in range(n_gx):
            base = (lax.rem(me_x + at, n_gx) * cols).astype(jnp.float32)
            factors(lax.broadcasted_iota(jnp.int32, (1, cols), 1).astype(jnp.float32) + base, cols)

            def write(to, value, at=at):
                tab[at, to, :] = value.astype(jnp.bfloat16)

            expand(write, cols)
            if part == 0 and at == 0:
                pl.when(jnp.logical_not(leads))(send_ahead)
        factors(lane.astype(jnp.float32) + float(nx), LANES)

        def write_zone(to, value):
            ztab[to, :] = jnp.where(lane < EXT_ZONE, value, 0.0).astype(jnp.bfloat16)

        expand(write_zone, LANES)

    t = jnp.minimum(lane + 1, EXT_ZONE).astype(jnp.float32) / (EXT_ZONE + 1.0)
    cube, square = t * t * t, t * t
    weight_a = 2.0 * cube - 3.0 * square + 1.0
    weight_b = cube - 2.0 * square + t
    weight_c = -2.0 * cube + 3.0 * square
    weight_d = cube - square
    tangent = EXT_ZONE + 1.0
    tail = cols - LANES

    def zone_of(parts):
        first = second = last = before = 0.0
        for at, part in enumerate(parts):
            owner = lax.rem(me_x + at, n_gx)
            is_first = jnp.where(owner == 0, 1.0, 0.0)
            is_last = jnp.where(owner == n_gx - 1, 1.0, 0.0)
            head = part[:, :LANES].astype(jnp.float32)
            rear = part[:, tail:].astype(jnp.float32)
            first += is_first * head[:, 0:1]
            second += is_first * head[:, 1:2]
            before += is_last * rear[:, LANES - 2:LANES - 1]
            last += is_last * rear[:, LANES - 1:LANES]
        zone = (last * weight_a + (tangent * (last - before)) * weight_b
                + first * weight_c + (tangent * (second - first)) * weight_d)
        return zone.astype(jnp.bfloat16)

    def dot(a, b):
        return lax.dot_general(a, b, NT, preferred_element_type=jnp.float32)

    def arrive(i):
        specs_in(i).wait_recv()
        for source in range(n_gy * n_gx):
            blk, level = place(i, source // n_gx)
            level += source % n_gx * share
            out_ref[source // n_gx * nblk + blk, pl.ds(level, bands, stride=levels), :] = (
                got[source, i].astype(jnp.float32))

    def own_part(i, part):
        blk, level = place(i, me_y)
        at = pl.ds(part * half, half)
        acc[at, :] = dot(tab[0, at, :], own[level, lines(blk), :])

    def blend(i):
        blk, level = place(i, me_y)
        at = lines(blk)
        zbuf[...] = zone_of([own[level, at, :]] + [xgot[x, level, at, :] for x in range(n_gx - 1)])

    def finish(i, lo, hi):
        blk, level = place(i, me_y)
        at = pl.ds(lo * bands, (hi - lo) * bands)
        total = acc[at, :] + dot(ztab[at, :], zbuf[...])
        for x in range(1, n_gx):
            total += dot(tab[x, at, :], xgot[x - 1, level, lines(blk), :])
        for b in range(lo, hi):
            piece = total[(b - lo) * bands:(b - lo + 1) * bands].astype(jnp.bfloat16)
            if b == len(blocks) - 1:
                got[me_y * n_gx + me_x, i] = piece
            else:
                send[b, i] = piece
                spec(b, i).start()

    def far_pieces(i):
        for lo in range(0, half // bands, n_gx):
            finish(i, lo, lo + n_gx)

    def near_pieces(i):
        finish(i, half // bands, len(blocks))

    def edges():
        top = me_y == 0
        row0 = pl.multiple_of(jnp.where(top, 0, rows - 16), 16)
        parts = [own[:, pl.ds(row0, 16), :].reshape(share * 16, cols)]
        parts += [xgot[x, :, pl.ds(row0, 16), :].reshape(share * 16, cols) for x in range(n_gx - 1)]
        total = dot(zone_of(parts), ztab[...])
        for x, part in enumerate(parts):
            total += dot(part, tab[x])
        esum[...] = total
        for pair in range(2):
            for level in range(share):
                upper = esum[level * 16 + pair:level * 16 + pair + 1, :]
                lower = esum[level * 16 + 14 + pair:level * 16 + 15 + pair, :]
                line = jnp.where(top, upper, lower)
                row = pair * share + level
                for b in range(len(blocks)):
                    esend[b, row:row + 1, :] = line[:, b * bands:(b + 1) * bands]
        for side, owner in ((0, 0), (1, n_gy - 1)):
            @pl.when(me_y == owner)
            def _(side=side):
                egot[side, me_x] = esend[len(blocks) - 1]
                for b in range(len(blocks) - 1):
                    edge(side, b).start()

    seam = (me_y == 0) | (me_y == n_gy - 1)

    def rows_ready(i):
        rows_in(i).wait_recv()

        @pl.when(i + depth < chunks)
        def _():
            for shift in range(1, n_gx):
                rows_x(shift, i + depth).start()

        blend(i)

    build(0)
    load(0).wait()
    own_part(0, 0)
    hear()
    rows_ready(0)
    far_pieces(0)
    build(1)
    own_part(0, 1)
    near_pieces(0)

    @pl.loop(1, chunks)
    def _(i):
        for turn_at in range(1, nblk):
            @pl.when(i == turn_at * share)
            def _():
                load(turn_at).wait()

        own_part(i, 0)
        own_part(i, 1)
        rows_ready(i)
        far_pieces(i)
        near_pieces(i)

        @pl.when(seam & (i == share - 1))
        def _():
            edges()

        @pl.when(i >= lag)
        def _():
            arrive(i - lag)

    for side, owner in ((0, 0), (1, n_gy - 1)):
        for x in range(n_gx):
            @pl.when((me_y != owner) | (me_x != x))
            def _(side=side, x=x):
                edge_in(side, x).wait_recv()

    pl.when(seam)(lambda: all_sent(esend.at[pl.ds(0, len(blocks) - 1)], fs))
    wa, wb, wc, wd = host_weights(EXT_ZONE)
    for x in range(n_gx):
        first, second = egot[0, x, :share, :], egot[0, x, share:, :]
        before, last = egot[1, x, :share, :], egot[1, x, share:, :]
        slope_start, slope_end = tangent * (last - before), tangent * (second - first)
        for j in range(EXT_ZONE):
            zone_ref[j, x * share:(x + 1) * share, :] = (
                last * float(wa[j]) + slope_start * float(wb[j])
                + first * float(wc[j]) + slope_end * float(wd[j]))

    for shift in range(1, n_gx):
        all_sent(field_ref.at[pl.ds(0, share)], xs.at[shift - 1])

    @pl.loop(chunks - lag, chunks)
    def _(i):
        arrive(i)

    all_sent(send, zs)


def make_fused_body(mesh):
    n_gx, n_gy = mesh.shape["gx"], mesh.shape["gy"]

    def body(field):
        levels, rows, cols = field.shape
        bands = cols // n_gy
        nblk, ny, size = rows // ROWS, rows * n_gy, n_gy * n_gx * bands
        share, xs, peers = levels // n_gx, n_gx - 1, n_gy * n_gx - 1
        chunks = share * nblk
        vmem, dma = pl.BlockSpec(memory_space=pltpu.VMEM), pltpu.SemaphoreType.DMA
        bf16, f32 = jnp.bfloat16, jnp.float32
        spectra, zone = pl.pallas_call(
            functools.partial(fused_kernel, n_gx, n_gy, depth=DEPTH, lags=(LAG_LEAD, LAG)),
            out_shape=(
                jax.ShapeDtypeStruct((n_gy * nblk, bands * levels, ROWS), f32),
                jax.ShapeDtypeStruct((EXT_ZONE, levels, bands), f32),
            ),
            in_specs=[pl.BlockSpec(memory_space=pltpu.HBM)],
            out_specs=(vmem, vmem),
            scratch_shapes=[
                pltpu.VMEM((share, rows, cols), bf16),
                pltpu.VMEM((xs, share, rows, cols), bf16),
                pltpu.VMEM((peers + 1, chunks, bands, ROWS), bf16),
                pltpu.VMEM((peers, chunks, bands, ROWS), bf16),
                pltpu.VMEM((n_gx, size, cols), bf16),
                pltpu.VMEM((size, LANES), bf16),
                pltpu.VMEM((ROWS, LANES), bf16),
                pltpu.VMEM((2, size // 2 // GROUP, cols), f32),
                pltpu.VMEM((2, GROUP, cols), f32),
                pltpu.VMEM((size, ROWS), f32),
                pltpu.VMEM((share * 16, size), f32),
                pltpu.VMEM((peers + 1, 2 * share, bands), f32),
                pltpu.VMEM((2, n_gx, 2 * share, bands), f32),
                dma((nblk,)), dma((xs,)), dma((chunks,)), dma, dma((chunks,)),
                dma, dma((2, n_gx)), pltpu.SemaphoreType.REGULAR((3,)),
            ],
            compiler_params=pltpu.CompilerParams(
                collective_id=0, has_side_effects=True, vmem_limit_bytes=VMEM_LIMIT),
        )(pltpu.with_memory_space_constraint(field, pltpu.HBM))
        spectra, zone = pl.pallas_call(
            store_kernel,
            out_shape=(
                jax.ShapeDtypeStruct((bands * levels, ny), f32),
                jax.ShapeDtypeStruct(zone.shape, f32),
            ),
            in_specs=[vmem, vmem],
            out_specs=(pl.BlockSpec(memory_space=pl.ANY),) * 2,
            scratch_shapes=[dma((n_gy * nblk + 1,))],
            compiler_params=pltpu.CompilerParams(vmem_limit_bytes=VMEM_LIMIT_STORE),
        )(spectra, zone)
        return spectra.reshape(bands, levels, ny), zone.transpose(2, 1, 0)

    return body


def store_kernel(tile_ref, zone_ref, out_ref, zone_out_ref, sem):
    count = tile_ref.shape[0]
    copies = [
        pltpu.make_async_copy(tile_ref.at[b], out_ref.at[:, pl.ds(b * ROWS, ROWS)], sem.at[b])
        for b in range(count)
    ]
    copies.append(pltpu.make_async_copy(zone_ref, zone_out_ref, sem.at[count]))
    for copy in copies:
        copy.start()
    for copy in copies:
        copy.wait()


VMEM_LIMIT_STORE = 16 * 2**20
DEPTH = 3
LAG_LEAD = 1
LAG = 3
VMEM_LIMIT = 36 * 2**20


def fits(mesh, shape):
    n_gx, n_gy = mesh.shape["gx"], mesh.shape["gy"]
    levels = shape[0] // (mesh.shape["member"] * mesh.shape["lev"])
    rows, cols = shape[1] // n_gy, shape[2] // n_gx
    bands = cols // n_gy
    return (n_gx > 1 and n_gy > 1 and n_gy % 2 == 0 and rows % ROWS == 0 and cols % LANES == 0
            and bands % GROUP == 0 and n_gy * n_gx * bands % (16 * GROUP) == 0
            and (cols * n_gx // 2) % bands == 0 and levels % 8 == 0 and levels % (2 * n_gx) == 0
            and levels // n_gx * rows // ROWS > max(DEPTH, LAG))


def solution(mesh):
    def program(field):
        body = make_fused_body(mesh) if fits(mesh, field.shape) else make_plain_body(mesh)
        return jax.shard_map(
            body,
            mesh=mesh,
            in_specs=(P(("member", "lev"), "gy", "gx"),),
            out_specs=(
                P(("gy", "gx"), ("member", "lev"), None),
                P(("gy", "gx"), ("member", "lev"), None),
            ),
            check_vma=False,
        )(field)

    return program
```

```python
import functools
import math

import jax
import jax.numpy as jnp
import numpy as np
from jax import lax
from jax.experimental import pallas as pl
from jax.experimental.pallas import tpu as pltpu
from jax.sharding import PartitionSpec as P

EXT_ZONE = 11
LANES = 128
NT = (((1,), (1,)), ((), ()))
MESH = pl.DeviceIdType.MESH


def blend_weights(zone_count):
    steps = (jnp.arange(zone_count, dtype=jnp.int32) + 1).astype(jnp.float32) / (zone_count + 1.0)
    weight_a = 2.0 * steps**3 - 3.0 * steps**2 + 1.0
    weight_b = steps**3 - 2.0 * steps**2 + steps
    weight_c = -2.0 * steps**3 + 3.0 * steps**2
    weight_d = steps**3 - steps**2
    return weight_a, weight_b, weight_c, weight_d


def blend_zone(second_last, last_value, first_value, second_value, zone_count):
    weight_a, weight_b, weight_c, weight_d = blend_weights(zone_count)
    tangent_scale = zone_count + 1.0
    slope_start = tangent_scale * (last_value - second_last)
    slope_end = tangent_scale * (second_value - first_value)
    return (
        last_value[..., None] * weight_a
        + slope_start[..., None] * weight_b
        + first_value[..., None] * weight_c
        + slope_end[..., None] * weight_d
    )


def wave_factors(coeff0, group, column, wave_count, length):
    number0 = jnp.where(coeff0 < wave_count, coeff0, coeff0 - wave_count + 1)
    scale = 2.0 * math.pi / length
    phase0 = (number0[:, None] * column[None, :] % length).astype(jnp.float32) * scale
    cos0, sin0 = jnp.cos(phase0), jnp.sin(phase0)
    is_cosine = (coeff0 < wave_count)[:, None]
    p, q = jnp.where(is_cosine, cos0, -sin0), jnp.where(is_cosine, sin0, cos0)
    step = jnp.arange(group, dtype=jnp.int32)
    phase = (step[:, None] * column[None, :] % length).astype(jnp.float32) * scale
    norm = 1.0 / math.sqrt(length)
    return p, q, jnp.cos(phase) * norm, jnp.sin(phase) * norm


def kernel(n_gx, n_gy, field_ref, edge_ref, table_ref, ztable_ref, weight_ref,
           out_ref, out_edge_ref, xgot, xedge, send, esend, xs, xr, es, er, zs, zr, ts, tr):
    levels, rows, cols = field_ref.shape
    bands = table_ref.shape[2]
    me_x, me_y = lax.axis_index("gx"), lax.axis_index("gy")

    def peer_x(shift):
        return {"gx": lax.rem(me_x + n_gx - shift, n_gx)}

    def peer_y(shift):
        return {"gy": lax.rem(me_y + shift, n_gy)}

    barrier = pltpu.get_barrier_semaphore()
    for shift in range(1, n_gx):
        pl.semaphore_signal(barrier, inc=1, device_id=peer_x(shift), device_id_type=MESH)
    for shift in range(1, n_gy):
        pl.semaphore_signal(barrier, inc=1, device_id=peer_y(shift), device_id_type=MESH)
    pl.semaphore_wait(barrier, n_gx + n_gy - 2)

    def edge_x(shift):
        return pltpu.make_async_remote_copy(
            src_ref=edge_ref, dst_ref=xedge.at[shift - 1], send_sem=es.at[shift - 1],
            recv_sem=er.at[shift - 1], device_id=peer_x(shift), device_id_type=MESH)

    def rows_x(shift, level):
        return pltpu.make_async_remote_copy(
            src_ref=field_ref.at[level], dst_ref=xgot.at[shift - 1, level],
            send_sem=xs.at[shift - 1, level], recv_sem=xr.at[shift - 1, level],
            device_id=peer_x(shift), device_id_type=MESH)

    def edge_y(shift):
        return pltpu.make_async_remote_copy(
            src_ref=esend.at[shift - 1], dst_ref=out_edge_ref.at[shift], send_sem=ts.at[shift - 1],
            recv_sem=tr.at[shift - 1], device_id=peer_y(shift), device_id_type=MESH)

    def spec_y(shift, level):
        return pltpu.make_async_remote_copy(
            src_ref=send.at[shift - 1, level], dst_ref=out_ref.at[shift, level],
            send_sem=zs.at[shift - 1, level], recv_sem=zr.at[shift - 1, level],
            device_id=peer_y(shift), device_id_type=MESH)

    for shift in range(1, n_gx):
        edge_x(shift).start()

    @pl.loop(0, levels)
    def _(level):
        for shift in range(1, n_gx):
            rows_x(shift, level).start()

    tail = (cols - 1) // LANES * LANES

    def zone_of(parts):
        first = second = last = before = 0.0
        for at, part in enumerate(parts):
            owner = lax.rem(me_x + at, n_gx)
            is_first = jnp.where(owner == 0, 1.0, 0.0)
            is_last = jnp.where(owner == n_gx - 1, 1.0, 0.0)
            head = part[:, :min(LANES, cols)].astype(jnp.float32)
            rear = part[:, tail:].astype(jnp.float32)
            first += is_first * head[:, 0:1]
            second += is_first * head[:, 1:2]
            before += is_last * rear[:, cols - 2 - tail:cols - 1 - tail]
            last += is_last * rear[:, cols - 1 - tail:cols - tail]
        tangent = EXT_ZONE + 1.0
        zone = (last * weight_ref[0:1, :] + (tangent * (last - before)) * weight_ref[1:2, :]
                + first * weight_ref[2:3, :] + (tangent * (second - first)) * weight_ref[3:4, :])
        return zone.astype(jnp.bfloat16)

    def dot(a, b):
        return lax.dot_general(a, b, NT, preferred_element_type=jnp.float32)

    for shift in range(1, n_gx):
        edge_x(shift).wait_recv()
    parts = [edge_ref[...]] + [xedge[at] for at in range(n_gx - 1)]
    zone = zone_of(parts)
    for shift in range(n_gy):
        total = dot(zone, ztable_ref[shift])
        for at, part in enumerate(parts):
            total += dot(part, table_ref[at, shift])
        if shift == 0:
            out_edge_ref[0] = total
        else:
            esend[shift - 1] = total
            edge_y(shift).start()

    merged = bands % 16 == 0

    @pl.loop(0, levels)
    def _(level):
        for shift in range(1, n_gx):
            rows_x(shift, level).wait_recv()
        parts = [field_ref[level]] + [xgot[at, level] for at in range(n_gx - 1)]
        zone = zone_of(parts)
        if merged:
            size = n_gy * bands
            total = dot(ztable_ref[...].reshape(size, LANES), zone)
            for at, part in enumerate(parts):
                total += dot(table_ref[at].reshape(size, cols), part)
            pieces = [total[s * bands:(s + 1) * bands] for s in range(n_gy)]
        else:
            pieces = []
            for shift in range(n_gy):
                total = dot(ztable_ref[shift], zone)
                for at, part in enumerate(parts):
                    total += dot(table_ref[at, shift], part)
                pieces.append(total)
        for shift in range(n_gy):
            piece = pieces[shift].astype(jnp.bfloat16)
            if shift == 0:
                out_ref[0, level] = piece
            else:
                send[shift - 1, level] = piece
        for shift in range(1, n_gy):
            spec_y(shift, level).start()

    for shift in range(1, n_gx):
        edge_x(shift).wait_send()
    for shift in range(1, n_gy):
        edge_y(shift).wait()

    @pl.loop(0, levels)
    def _(level):
        for shift in range(1, n_gx):
            rows_x(shift, level).wait_send()
        for shift in range(1, n_gy):
            spec_y(shift, level).wait()


def make_plain_body(mesh):
    n_gx, n_gy = mesh.shape["gx"], mesh.shape["gy"]

    def body(field):
        levels, rows, cols = field.shape
        nx, ny = cols * n_gx, rows * n_gy
        length = nx + EXT_ZONE
        me_x, me_y = lax.axis_index("gx"), lax.axis_index("gy")
        bands = nx // (n_gx * n_gy)
        assert (nx // 2) % bands == 0
        group = 16 if bands % 16 == 0 else bands

        at = jnp.arange(nx + LANES, dtype=jnp.int32)
        column = jnp.where(at < nx, (at + me_x * cols) % nx, at)
        shift_at = jnp.arange(n_gy, dtype=jnp.int32)[:, None]
        coeff = ((me_y + shift_at) % n_gy) * (n_gx * bands) + me_x * bands
        coeff = (coeff + jnp.arange(0, bands, group, dtype=jnp.int32)[None, :]).reshape(-1)
        factors = wave_factors(coeff, group, column, nx // 2, length)
        p, q, c, s = lax.optimization_barrier(factors)

        def expand(lo, hi):
            full = p[:, None, lo:hi] * c[None, :, lo:hi] - q[:, None, lo:hi] * s[None, :, lo:hi]
            return full.astype(jnp.bfloat16).reshape(n_gy, bands, hi - lo)

        table = jnp.stack([expand(i * cols, (i + 1) * cols) for i in range(n_gx)])
        ztable = expand(nx, nx + LANES)
        ztable = jnp.where(jnp.arange(LANES) < EXT_ZONE, ztable, jnp.zeros_like(ztable))
        weights = jnp.pad(jnp.stack(blend_weights(EXT_ZONE)), ((0, 4), (0, LANES - EXT_ZONE)))
        edge = jnp.concatenate([field[:, :2], field[:, rows - 2:]], axis=1)
        edge = edge.transpose(1, 0, 2).reshape(4 * levels, cols)

        vmem = pl.BlockSpec(memory_space=pltpu.VMEM)
        dma = pltpu.SemaphoreType.DMA
        xs, ys = n_gx - 1, n_gy - 1
        got, edge_got = pl.pallas_call(
            functools.partial(kernel, n_gx, n_gy),
            out_shape=(
                jax.ShapeDtypeStruct((n_gy, levels, bands, rows), jnp.bfloat16),
                jax.ShapeDtypeStruct((n_gy, 4 * levels, bands), jnp.float32),
            ),
            in_specs=[vmem] * 5,
            out_specs=(vmem, vmem),
            scratch_shapes=[
                pltpu.VMEM((xs, levels, rows, cols), jnp.bfloat16),
                pltpu.VMEM((xs, 4 * levels, cols), jnp.bfloat16),
                pltpu.VMEM((ys, levels, bands, rows), jnp.bfloat16),
                pltpu.VMEM((ys, 4 * levels, bands), jnp.float32),
                dma((xs, levels)), dma((xs, levels)), dma((xs,)), dma((xs,)),
                dma((ys, levels)), dma((ys, levels)), dma((ys,)), dma((ys,)),
            ],
            compiler_params=pltpu.CompilerParams(collective_id=0, has_side_effects=True),
        )(field, edge, table, ztable, weights)

        edge_got = edge_got.reshape(n_gy, 4, levels, bands)
        low = lax.dynamic_index_in_dim(edge_got, me_y, 0, keepdims=False)
        high = lax.dynamic_index_in_dim(edge_got, (me_y + 1) % n_gy, 0, keepdims=False)
        low, high = low.transpose(0, 2, 1), high.transpose(0, 2, 1)
        spectra_zone = blend_zone(high[2], high[3], low[0], low[1], EXT_ZONE)

        spectra = jnp.zeros((bands, levels, ny), jnp.float32)
        for shift in range(n_gy):
            full = got[shift].transpose(1, 0, 2).astype(jnp.float32)
            source = (me_y + n_gy - shift) % n_gy
            spectra = lax.dynamic_update_slice(spectra, full, (0, 0, source * rows))
        return spectra, spectra_zone

    return body


ROWS = 128
GROUP = 16


def host_weights(zone_count):
    t = (np.arange(zone_count, dtype=np.float32) + np.float32(1)) / np.float32(zone_count + 1.0)
    two, three, one = np.float32(2), np.float32(3), np.float32(1)
    cube, square = t * t * t, t * t
    return (two * cube - three * square + one, cube - two * square + t,
            three * square - two * cube, cube - square)


def unit_circle(product, length):
    quarter = length / 4.0
    turns = jnp.floor(product * (4.0 / length) + 0.5)
    theta = (product - turns * quarter) * (2.0 * math.pi / length)
    turns = turns - 4.0 * jnp.floor(turns * 0.25)
    z = theta * theta
    sin = theta * (1.0 + z * (-1.0 / 6 + z * (1.0 / 120 + z * (-1.0 / 5040 + z * (1.0 / 362880)))))
    cos = 1.0 + z * (-0.5 + z * (1.0 / 24 + z * (-1.0 / 720 + z * (1.0 / 40320 - z * (1.0 / 3628800)))))
    odd = (turns == 1.0) | (turns == 3.0)
    c, s = jnp.where(odd, sin, cos), jnp.where(odd, cos, sin)
    c = jnp.where((turns == 1.0) | (turns == 2.0), -c, c)
    s = jnp.where(turns >= 2.0, -s, s)
    return c, s


def fused_kernel(n_gx, n_gy, field_ref, out_ref, zone_ref,
                 own, staged, xgot, got, send, tab, ztab, zbuf, pq, cs, acc, esum, esend, egot,
                 ss, ls, xs, xr, zs, zr, fs, fr, far, *, depth, lags):
    levels, rows, cols = field_ref.shape
    bands = got.shape[2]
    nblk, share = rows // ROWS, levels // n_gx
    half = n_gy // 2 * n_gx * bands
    nx = n_gx * cols
    length = nx + EXT_ZONE
    me_x, me_y = lax.axis_index("gx"), lax.axis_index("gy")
    chunks = share * nblk
    blocks = [(k, x) for k in range(n_gy - 1) for x in range(n_gx)]
    blocks += [(n_gy - 1, x) for x in range(1, n_gx)] + [(n_gy - 1, 0)]

    def peer_x(shift):
        return {"gx": lax.rem(me_x + n_gx - shift, n_gx)}

    def peer_y(shift):
        return {"gy": lax.rem(me_y + shift, n_gy)}

    def turn(k):
        up, down = n_gy - 1 - k, k
        if k == n_gy - 1:
            return 0
        up = jnp.where(up > me_y, up, up - 1)
        down = jnp.where(down < me_y, down, down + 1)
        return lax.rem(jnp.where(2 * me_y < n_gy, up, down) - me_y + n_gy, n_gy)

    above, below = me_y < n_gy - 1, me_y > 0

    def tell(semaphore, up):
        pl.semaphore_signal(semaphore, inc=1, device_id={"gy": me_y + (1 if up else -1)},
                            device_id_type=MESH)

    barrier = pltpu.get_barrier_semaphore()
    for shift in range(1, n_gx):
        pl.semaphore_signal(barrier, inc=1, device_id=peer_x(shift), device_id_type=MESH)
    pl.when(above)(lambda: tell(barrier, True))
    pl.when(below)(lambda: tell(barrier, False))

    def vouch():
        pl.when(above & below)(lambda: tell(far.at[0], False))
        pl.when(above & below)(lambda: tell(far.at[1], True))

    def hear():
        for hop in range(n_gy - 2):
            @pl.when(me_y + hop < n_gy - 2)
            def _():
                pl.semaphore_wait(far.at[0], 1)
                pl.when(below)(lambda: tell(far.at[0], False))

            @pl.when(me_y - hop > 1)
            def _():
                pl.semaphore_wait(far.at[1], 1)
                pl.when(above)(lambda: tell(far.at[1], True))

        for shift in range(1, n_gx):
            pl.semaphore_signal(far.at[2], inc=1, device_id=peer_x(shift), device_id_type=MESH)
        pl.semaphore_wait(far.at[2], n_gx - 1)

    def place(i, owner):
        ahead = jnp.where(owner == n_gy - 1, nblk - 1, 0)
        return lax.rem(i // share + ahead, nblk), lax.rem(i, share)

    def lines(blk):
        return pl.ds(pl.multiple_of(blk * ROWS, ROWS), ROWS)

    def load(turn_at):
        blk, _ = place(turn_at * share, me_y)
        at = lines(blk)
        return pltpu.make_async_copy(
            field_ref.at[pl.ds(me_x * share, share), at], own.at[:, at], ls.at[turn_at])

    def stage(shift):
        blk, _ = place(0, me_y)
        return pltpu.make_async_copy(
            field_ref.at[peer_x(shift)["gx"] * share, lines(blk)], staged.at[shift - 1], ss.at[shift - 1])

    def rows_x(shift, i, source=None):
        blk, level = place(i, me_y)
        at = lines(blk)
        peer = peer_x(shift)
        if source is None:
            source = field_ref.at[peer["gx"] * share + level, at]
        return pltpu.make_async_remote_copy(
            src_ref=source, dst_ref=xgot.at[shift - 1, level, at],
            send_sem=xs.at[shift - 1], recv_sem=xr.at[i], device_id=peer, device_id_type=MESH)

    def rows_in(i):
        blk, level = place(i, me_y)
        ref = xgot.at[:, level, lines(blk)]
        return pltpu.make_async_remote_copy(
            src_ref=ref, dst_ref=ref, send_sem=xs.at[0], recv_sem=xr.at[i],
            device_id=peer_x(1), device_id_type=MESH)

    def owner_of(b):
        k, x = blocks[b]
        return {"gy": lax.rem(me_y + turn(k), n_gy), "gx": lax.rem(me_x + x, n_gx)}

    def spec(b, i):
        return pltpu.make_async_remote_copy(
            src_ref=send.at[b, i], dst_ref=got.at[me_y * n_gx + me_x, i],
            send_sem=zs, recv_sem=zr.at[i], device_id=owner_of(b), device_id_type=MESH)

    def specs_in(i):
        return pltpu.make_async_remote_copy(
            src_ref=send.at[:, 0], dst_ref=got.at[pl.ds(0, len(blocks) - 1), 0],
            send_sem=zs, recv_sem=zr.at[i], device_id=peer_y(1), device_id_type=MESH)

    def edge(side, b):
        return pltpu.make_async_remote_copy(
            src_ref=esend.at[b], dst_ref=egot.at[side, me_x], send_sem=fs, recv_sem=fr.at[side, me_x],
            device_id=owner_of(b), device_id_type=MESH)

    def edge_in(side, x):
        return pltpu.make_async_remote_copy(
            src_ref=esend.at[0], dst_ref=egot.at[side, x], send_sem=fs, recv_sem=fr.at[side, x],
            device_id=peer_y(1), device_id_type=MESH)

    def all_sent(ref, semaphore):
        pltpu.make_async_remote_copy(
            src_ref=ref, dst_ref=ref, send_sem=semaphore, recv_sem=fr.at[0, 0],
            device_id=peer_y(1), device_id_type=MESH).wait_send()

    for shift in range(1, n_gx):
        stage(shift).start()
    for turn_at in range(nblk):
        load(turn_at).start()

    pl.semaphore_wait(barrier, n_gx - 1 + above.astype(jnp.int32) + below.astype(jnp.int32))

    def send_ahead():
        for shift in range(1, n_gx):
            stage(shift).wait()
            rows_x(shift, 0, staged.at[shift - 1]).start()

        @pl.loop(1, depth)
        def _(i):
            for shift in range(1, n_gx):
                rows_x(shift, i).start()

    leads = lax.axis_index("lev") != 0
    lag = jnp.where(leads, *lags)
    pl.when(leads)(send_ahead)
    vouch()

    norm = 1.0 / math.sqrt(length)
    ngroup = half // GROUP
    lane = lax.broadcasted_iota(jnp.int32, (1, LANES), 1)

    def build(part):
        row0 = part * half
        g = lax.broadcasted_iota(jnp.int32, (ngroup, 1), 0) * GROUP + row0
        block = g // bands
        origin = jnp.zeros((ngroup, 1), jnp.int32)
        for b in range(row0 // bands, (row0 + half) // bands):
            to = owner_of(b)
            origin = jnp.where(block == b, (to["gy"] * n_gx + to["gx"]) * bands, origin)
        first = origin + (g - block * bands)
        is_cos = first < nx // 2
        number = jnp.where(is_cos, first, first - (nx // 2 - 1)).astype(jnp.float32)
        step = lax.broadcasted_iota(jnp.int32, (GROUP, 1), 0).astype(jnp.float32)

        def factors(column, width):
            c, s = unit_circle(number * column, length)
            pq[0, :, :width], pq[1, :, :width] = jnp.where(is_cos, c, -s), jnp.where(is_cos, s, c)
            c, s = unit_circle(step * column, length)
            cs[0, :, :width], cs[1, :, :width] = c * norm, s * norm

        def expand(write, width):
            @pl.loop(0, ngroup // 8)
            def _(k):
                at = pl.ds(pl.multiple_of(k * 8, 8), 8)
                for r in range(8):
                    p, q = pq[0, at, :width][r:r + 1], pq[1, at, :width][r:r + 1]
                    write(pl.ds(pl.multiple_of(row0 + (k * 8 + r) * GROUP, GROUP), GROUP),
                          p * cs[0, :, :width] - q * cs[1, :, :width])

        for at in range(n_gx):
            base = (lax.rem(me_x + at, n_gx) * cols).astype(jnp.float32)
            factors(lax.broadcasted_iota(jnp.int32, (1, cols), 1).astype(jnp.float32) + base, cols)

            def write(to, value, at=at):
                tab[at, to, :] = value.astype(jnp.bfloat16)

            expand(write, cols)
            if part == 0 and at == 0:
                pl.when(jnp.logical_not(leads))(send_ahead)
        factors(lane.astype(jnp.float32) + float(nx), LANES)

        def write_zone(to, value):
            ztab[to, :] = jnp.where(lane < EXT_ZONE, value, 0.0).astype(jnp.bfloat16)

        expand(write_zone, LANES)

    t = jnp.minimum(lane + 1, EXT_ZONE).astype(jnp.float32) / (EXT_ZONE + 1.0)
    cube, square = t * t * t, t * t
    weight_a = 2.0 * cube - 3.0 * square + 1.0
    weight_b = cube - 2.0 * square + t
    weight_c = -2.0 * cube + 3.0 * square
    weight_d = cube - square
    tangent = EXT_ZONE + 1.0
    tail = cols - LANES

    def zone_of(parts):
        first = second = last = before = 0.0
        for at, part in enumerate(parts):
            owner = lax.rem(me_x + at, n_gx)
            is_first = jnp.where(owner == 0, 1.0, 0.0)
            is_last = jnp.where(owner == n_gx - 1, 1.0, 0.0)
            head = part[:, :LANES].astype(jnp.float32)
            rear = part[:, tail:].astype(jnp.float32)
            first += is_first * head[:, 0:1]
            second += is_first * head[:, 1:2]
            before += is_last * rear[:, LANES - 2:LANES - 1]
            last += is_last * rear[:, LANES - 1:LANES]
        zone = (last * weight_a + (tangent * (last - before)) * weight_b
                + first * weight_c + (tangent * (second - first)) * weight_d)
        return zone.astype(jnp.bfloat16)

    def dot(a, b):
        return lax.dot_general(a, b, NT, preferred_element_type=jnp.float32)

    def arrive(i):
        specs_in(i).wait_recv()
        for source in range(n_gy * n_gx):
            blk, level = place(i, source // n_gx)
            level += source % n_gx * share
            out_ref[source // n_gx * nblk + blk, pl.ds(level, bands, stride=levels), :] = (
                got[source, i].astype(jnp.float32))

    def own_part(i, part):
        blk, level = place(i, me_y)
        at = pl.ds(part * half, half)
        acc[at, :] = dot(tab[0, at, :], own[level, lines(blk), :])

    def blend(i):
        blk, level = place(i, me_y)
        at = lines(blk)
        zbuf[...] = zone_of([own[level, at, :]] + [xgot[x, level, at, :] for x in range(n_gx - 1)])

    def finish(i, lo, hi):
        blk, level = place(i, me_y)
        at = pl.ds(lo * bands, (hi - lo) * bands)
        total = acc[at, :] + dot(ztab[at, :], zbuf[...])
        for x in range(1, n_gx):
            total += dot(tab[x, at, :], xgot[x - 1, level, lines(blk), :])
        for b in range(lo, hi):
            piece = total[(b - lo) * bands:(b - lo + 1) * bands].astype(jnp.bfloat16)
            if b == len(blocks) - 1:
                got[me_y * n_gx + me_x, i] = piece
            else:
                send[b, i] = piece
                spec(b, i).start()

    def far_pieces(i):
        for lo in range(0, half // bands, n_gx):
            finish(i, lo, lo + n_gx)

    def near_pieces(i):
        finish(i, half // bands, len(blocks))

    def edges():
        top = me_y == 0
        row0 = pl.multiple_of(jnp.where(top, 0, rows - 16), 16)
        parts = [own[:, pl.ds(row0, 16), :].reshape(share * 16, cols)]
        parts += [xgot[x, :, pl.ds(row0, 16), :].reshape(share * 16, cols) for x in range(n_gx - 1)]
        total = dot(zone_of(parts), ztab[...])
        for x, part in enumerate(parts):
            total += dot(part, tab[x])
        esum[...] = total
        for pair in range(2):
            for level in range(share):
                upper = esum[level * 16 + pair:level * 16 + pair + 1, :]
                lower = esum[level * 16 + 14 + pair:level * 16 + 15 + pair, :]
                line = jnp.where(top, upper, lower)
                row = pair * share + level
                for b in range(len(blocks)):
                    esend[b, row:row + 1, :] = line[:, b * bands:(b + 1) * bands]
        for side, owner in ((0, 0), (1, n_gy - 1)):
            @pl.when(me_y == owner)
            def _(side=side):
                egot[side, me_x] = esend[len(blocks) - 1]
                for b in range(len(blocks) - 1):
                    edge(side, b).start()

    seam = (me_y == 0) | (me_y == n_gy - 1)

    def rows_ready(i):
        rows_in(i).wait_recv()

        @pl.when(i + depth < chunks)
        def _():
            for shift in range(1, n_gx):
                rows_x(shift, i + depth).start()

        blend(i)

    build(0)
    load(0).wait()
    own_part(0, 0)
    hear()
    rows_ready(0)
    far_pieces(0)
    build(1)
    own_part(0, 1)
    near_pieces(0)

    @pl.loop(1, chunks)
    def _(i):
        for turn_at in range(1, nblk):
            @pl.when(i == turn_at * share)
            def _():
                load(turn_at).wait()

        own_part(i, 0)
        own_part(i, 1)
        rows_ready(i)
        far_pieces(i)
        near_pieces(i)

        @pl.when(seam & (i == share - 1))
        def _():
            edges()

        @pl.when(i >= lag)
        def _():
            arrive(i - lag)

    for side, owner in ((0, 0), (1, n_gy - 1)):
        for x in range(n_gx):
            @pl.when((me_y != owner) | (me_x != x))
            def _(side=side, x=x):
                edge_in(side, x).wait_recv()

    pl.when(seam)(lambda: all_sent(esend.at[pl.ds(0, len(blocks) - 1)], fs))
    wa, wb, wc, wd = host_weights(EXT_ZONE)
    for x in range(n_gx):
        first, second = egot[0, x, :share, :], egot[0, x, share:, :]
        before, last = egot[1, x, :share, :], egot[1, x, share:, :]
        slope_start, slope_end = tangent * (last - before), tangent * (second - first)
        for j in range(EXT_ZONE):
            zone_ref[j, x * share:(x + 1) * share, :] = (
                last * float(wa[j]) + slope_start * float(wb[j])
                + first * float(wc[j]) + slope_end * float(wd[j]))

    for shift in range(1, n_gx):
        all_sent(field_ref.at[pl.ds(0, share)], xs.at[shift - 1])

    @pl.loop(chunks - lag, chunks)
    def _(i):
        arrive(i)

    all_sent(send, zs)


def make_fused_body(mesh):
    n_gx, n_gy = mesh.shape["gx"], mesh.shape["gy"]

    def body(field):
        levels, rows, cols = field.shape
        bands = cols // n_gy
        nblk, ny, size = rows // ROWS, rows * n_gy, n_gy * n_gx * bands
        share, xs, peers = levels // n_gx, n_gx - 1, n_gy * n_gx - 1
        chunks = share * nblk
        vmem, dma = pl.BlockSpec(memory_space=pltpu.VMEM), pltpu.SemaphoreType.DMA
        bf16, f32 = jnp.bfloat16, jnp.float32
        spectra, zone = pl.pallas_call(
            functools.partial(fused_kernel, n_gx, n_gy, depth=DEPTH, lags=(LAG_LEAD, LAG)),
            out_shape=(
                jax.ShapeDtypeStruct((n_gy * nblk, bands * levels, ROWS), f32),
                jax.ShapeDtypeStruct((EXT_ZONE, levels, bands), f32),
            ),
            in_specs=[pl.BlockSpec(memory_space=pltpu.HBM)],
            out_specs=(vmem, vmem),
            scratch_shapes=[
                pltpu.VMEM((share, rows, cols), bf16),
                pltpu.VMEM((xs, ROWS, cols), bf16),
                pltpu.VMEM((xs, share, rows, cols), bf16),
                pltpu.VMEM((peers + 1, chunks, bands, ROWS), bf16),
                pltpu.VMEM((peers, chunks, bands, ROWS), bf16),
                pltpu.VMEM((n_gx, size, cols), bf16),
                pltpu.VMEM((size, LANES), bf16),
                pltpu.VMEM((ROWS, LANES), bf16),
                pltpu.VMEM((2, size // 2 // GROUP, cols), f32),
                pltpu.VMEM((2, GROUP, cols), f32),
                pltpu.VMEM((size, ROWS), f32),
                pltpu.VMEM((share * 16, size), f32),
                pltpu.VMEM((peers + 1, 2 * share, bands), f32),
                pltpu.VMEM((2, n_gx, 2 * share, bands), f32),
                dma((xs,)), dma((nblk,)), dma((xs,)), dma((chunks,)), dma, dma((chunks,)),
                dma, dma((2, n_gx)), pltpu.SemaphoreType.REGULAR((3,)),
            ],
            compiler_params=pltpu.CompilerParams(
                collective_id=0, has_side_effects=True, vmem_limit_bytes=VMEM_LIMIT),
        )(pltpu.with_memory_space_constraint(field, pltpu.HBM))
        spectra, zone = pl.pallas_call(
            store_kernel,
            out_shape=(
                jax.ShapeDtypeStruct((bands * levels, ny), f32),
                jax.ShapeDtypeStruct(zone.shape, f32),
            ),
            in_specs=[vmem, vmem],
            out_specs=(pl.BlockSpec(memory_space=pl.ANY),) * 2,
            scratch_shapes=[dma((n_gy * nblk + 1,))],
            compiler_params=pltpu.CompilerParams(vmem_limit_bytes=VMEM_LIMIT_STORE),
        )(spectra, zone)
        return spectra.reshape(bands, levels, ny), zone.transpose(2, 1, 0)

    return body


def store_kernel(tile_ref, zone_ref, out_ref, zone_out_ref, sem):
    count = tile_ref.shape[0]
    copies = [
        pltpu.make_async_copy(tile_ref.at[b], out_ref.at[:, pl.ds(b * ROWS, ROWS)], sem.at[b])
        for b in range(count)
    ]
    copies.append(pltpu.make_async_copy(zone_ref, zone_out_ref, sem.at[count]))
    for copy in copies:
        copy.start()
    for copy in copies:
        copy.wait()


VMEM_LIMIT_STORE = 16 * 2**20
DEPTH = 3
LAG_LEAD = 1
LAG = 3
VMEM_LIMIT = 36 * 2**20


def fits(mesh, shape):
    n_gx, n_gy = mesh.shape["gx"], mesh.shape["gy"]
    levels = shape[0] // (mesh.shape["member"] * mesh.shape["lev"])
    rows, cols = shape[1] // n_gy, shape[2] // n_gx
    bands = cols // n_gy
    return (n_gx > 1 and n_gy > 1 and n_gy % 2 == 0 and rows % ROWS == 0 and cols % LANES == 0
            and bands % GROUP == 0 and n_gy * n_gx * bands % (16 * GROUP) == 0
            and (cols * n_gx // 2) % bands == 0 and levels % 8 == 0 and levels % (2 * n_gx) == 0
            and levels // n_gx * rows // ROWS > max(DEPTH, LAG))


def solution(mesh):
    def program(field):
        body = make_fused_body(mesh) if fits(mesh, field.shape) else make_plain_body(mesh)
        return jax.shard_map(
            body,
            mesh=mesh,
            in_specs=(P(("member", "lev"), "gy", "gx"),),
            out_specs=(
                P(("gy", "gx"), ("member", "lev"), None),
                P(("gy", "gx"), ("member", "lev"), None),
            ),
            check_vma=False,
        )(field)

    return program
```

```python
import functools
import math

import jax
import jax.numpy as jnp
import numpy as np
from jax import lax
from jax.experimental import pallas as pl
from jax.experimental.pallas import tpu as pltpu
from jax.sharding import PartitionSpec as P

EXT_ZONE = 11
LANES = 128
NT = (((1,), (1,)), ((), ()))
MESH = pl.DeviceIdType.MESH


def blend_weights(zone_count):
    steps = (jnp.arange(zone_count, dtype=jnp.int32) + 1).astype(jnp.float32) / (zone_count + 1.0)
    weight_a = 2.0 * steps**3 - 3.0 * steps**2 + 1.0
    weight_b = steps**3 - 2.0 * steps**2 + steps
    weight_c = -2.0 * steps**3 + 3.0 * steps**2
    weight_d = steps**3 - steps**2
    return weight_a, weight_b, weight_c, weight_d


def blend_zone(second_last, last_value, first_value, second_value, zone_count):
    weight_a, weight_b, weight_c, weight_d = blend_weights(zone_count)
    tangent_scale = zone_count + 1.0
    slope_start = tangent_scale * (last_value - second_last)
    slope_end = tangent_scale * (second_value - first_value)
    return (
        last_value[..., None] * weight_a
        + slope_start[..., None] * weight_b
        + first_value[..., None] * weight_c
        + slope_end[..., None] * weight_d
    )


def wave_factors(coeff0, group, column, wave_count, length):
    number0 = jnp.where(coeff0 < wave_count, coeff0, coeff0 - wave_count + 1)
    scale = 2.0 * math.pi / length
    phase0 = (number0[:, None] * column[None, :] % length).astype(jnp.float32) * scale
    cos0, sin0 = jnp.cos(phase0), jnp.sin(phase0)
    is_cosine = (coeff0 < wave_count)[:, None]
    p, q = jnp.where(is_cosine, cos0, -sin0), jnp.where(is_cosine, sin0, cos0)
    step = jnp.arange(group, dtype=jnp.int32)
    phase = (step[:, None] * column[None, :] % length).astype(jnp.float32) * scale
    norm = 1.0 / math.sqrt(length)
    return p, q, jnp.cos(phase) * norm, jnp.sin(phase) * norm


def kernel(n_gx, n_gy, field_ref, edge_ref, table_ref, ztable_ref, weight_ref,
           out_ref, out_edge_ref, xgot, xedge, send, esend, xs, xr, es, er, zs, zr, ts, tr):
    levels, rows, cols = field_ref.shape
    bands = table_ref.shape[2]
    me_x, me_y = lax.axis_index("gx"), lax.axis_index("gy")

    def peer_x(shift):
        return {"gx": lax.rem(me_x + n_gx - shift, n_gx)}

    def peer_y(shift):
        return {"gy": lax.rem(me_y + shift, n_gy)}

    barrier = pltpu.get_barrier_semaphore()
    for shift in range(1, n_gx):
        pl.semaphore_signal(barrier, inc=1, device_id=peer_x(shift), device_id_type=MESH)
    for shift in range(1, n_gy):
        pl.semaphore_signal(barrier, inc=1, device_id=peer_y(shift), device_id_type=MESH)
    pl.semaphore_wait(barrier, n_gx + n_gy - 2)

    def edge_x(shift):
        return pltpu.make_async_remote_copy(
            src_ref=edge_ref, dst_ref=xedge.at[shift - 1], send_sem=es.at[shift - 1],
            recv_sem=er.at[shift - 1], device_id=peer_x(shift), device_id_type=MESH)

    def rows_x(shift, level):
        return pltpu.make_async_remote_copy(
            src_ref=field_ref.at[level], dst_ref=xgot.at[shift - 1, level],
            send_sem=xs.at[shift - 1, level], recv_sem=xr.at[shift - 1, level],
            device_id=peer_x(shift), device_id_type=MESH)

    def edge_y(shift):
        return pltpu.make_async_remote_copy(
            src_ref=esend.at[shift - 1], dst_ref=out_edge_ref.at[shift], send_sem=ts.at[shift - 1],
            recv_sem=tr.at[shift - 1], device_id=peer_y(shift), device_id_type=MESH)

    def spec_y(shift, level):
        return pltpu.make_async_remote_copy(
            src_ref=send.at[shift - 1, level], dst_ref=out_ref.at[shift, level],
            send_sem=zs.at[shift - 1, level], recv_sem=zr.at[shift - 1, level],
            device_id=peer_y(shift), device_id_type=MESH)

    for shift in range(1, n_gx):
        edge_x(shift).start()

    @pl.loop(0, levels)
    def _(level):
        for shift in range(1, n_gx):
            rows_x(shift, level).start()

    tail = (cols - 1) // LANES * LANES

    def zone_of(parts):
        first = second = last = before = 0.0
        for at, part in enumerate(parts):
            owner = lax.rem(me_x + at, n_gx)
            is_first = jnp.where(owner == 0, 1.0, 0.0)
            is_last = jnp.where(owner == n_gx - 1, 1.0, 0.0)
            head = part[:, :min(LANES, cols)].astype(jnp.float32)
            rear = part[:, tail:].astype(jnp.float32)
            first += is_first * head[:, 0:1]
            second += is_first * head[:, 1:2]
            before += is_last * rear[:, cols - 2 - tail:cols - 1 - tail]
            last += is_last * rear[:, cols - 1 - tail:cols - tail]
        tangent = EXT_ZONE + 1.0
        zone = (last * weight_ref[0:1, :] + (tangent * (last - before)) * weight_ref[1:2, :]
                + first * weight_ref[2:3, :] + (tangent * (second - first)) * weight_ref[3:4, :])
        return zone.astype(jnp.bfloat16)

    def dot(a, b):
        return lax.dot_general(a, b, NT, preferred_element_type=jnp.float32)

    for shift in range(1, n_gx):
        edge_x(shift).wait_recv()
    parts = [edge_ref[...]] + [xedge[at] for at in range(n_gx - 1)]
    zone = zone_of(parts)
    for shift in range(n_gy):
        total = dot(zone, ztable_ref[shift])
        for at, part in enumerate(parts):
            total += dot(part, table_ref[at, shift])
        if shift == 0:
            out_edge_ref[0] = total
        else:
            esend[shift - 1] = total
            edge_y(shift).start()

    merged = bands % 16 == 0

    @pl.loop(0, levels)
    def _(level):
        for shift in range(1, n_gx):
            rows_x(shift, level).wait_recv()
        parts = [field_ref[level]] + [xgot[at, level] for at in range(n_gx - 1)]
        zone = zone_of(parts)
        if merged:
            size = n_gy * bands
            total = dot(ztable_ref[...].reshape(size, LANES), zone)
            for at, part in enumerate(parts):
                total += dot(table_ref[at].reshape(size, cols), part)
            pieces = [total[s * bands:(s + 1) * bands] for s in range(n_gy)]
        else:
            pieces = []
            for shift in range(n_gy):
                total = dot(ztable_ref[shift], zone)
                for at, part in enumerate(parts):
                    total += dot(table_ref[at, shift], part)
                pieces.append(total)
        for shift in range(n_gy):
            piece = pieces[shift].astype(jnp.bfloat16)
            if shift == 0:
                out_ref[0, level] = piece
            else:
                send[shift - 1, level] = piece
        for shift in range(1, n_gy):
            spec_y(shift, level).start()

    for shift in range(1, n_gx):
        edge_x(shift).wait_send()
    for shift in range(1, n_gy):
        edge_y(shift).wait()

    @pl.loop(0, levels)
    def _(level):
        for shift in range(1, n_gx):
            rows_x(shift, level).wait_send()
        for shift in range(1, n_gy):
            spec_y(shift, level).wait()


def make_plain_body(mesh):
    n_gx, n_gy = mesh.shape["gx"], mesh.shape["gy"]

    def body(field):
        levels, rows, cols = field.shape
        nx, ny = cols * n_gx, rows * n_gy
        length = nx + EXT_ZONE
        me_x, me_y = lax.axis_index("gx"), lax.axis_index("gy")
        bands = nx // (n_gx * n_gy)
        assert (nx // 2) % bands == 0
        group = 16 if bands % 16 == 0 else bands

        at = jnp.arange(nx + LANES, dtype=jnp.int32)
        column = jnp.where(at < nx, (at + me_x * cols) % nx, at)
        shift_at = jnp.arange(n_gy, dtype=jnp.int32)[:, None]
        coeff = ((me_y + shift_at) % n_gy) * (n_gx * bands) + me_x * bands
        coeff = (coeff + jnp.arange(0, bands, group, dtype=jnp.int32)[None, :]).reshape(-1)
        factors = wave_factors(coeff, group, column, nx // 2, length)
        p, q, c, s = lax.optimization_barrier(factors)

        def expand(lo, hi):
            full = p[:, None, lo:hi] * c[None, :, lo:hi] - q[:, None, lo:hi] * s[None, :, lo:hi]
            return full.astype(jnp.bfloat16).reshape(n_gy, bands, hi - lo)

        table = jnp.stack([expand(i * cols, (i + 1) * cols) for i in range(n_gx)])
        ztable = expand(nx, nx + LANES)
        ztable = jnp.where(jnp.arange(LANES) < EXT_ZONE, ztable, jnp.zeros_like(ztable))
        weights = jnp.pad(jnp.stack(blend_weights(EXT_ZONE)), ((0, 4), (0, LANES - EXT_ZONE)))
        edge = jnp.concatenate([field[:, :2], field[:, rows - 2:]], axis=1)
        edge = edge.transpose(1, 0, 2).reshape(4 * levels, cols)

        vmem = pl.BlockSpec(memory_space=pltpu.VMEM)
        dma = pltpu.SemaphoreType.DMA
        xs, ys = n_gx - 1, n_gy - 1
        got, edge_got = pl.pallas_call(
            functools.partial(kernel, n_gx, n_gy),
            out_shape=(
                jax.ShapeDtypeStruct((n_gy, levels, bands, rows), jnp.bfloat16),
                jax.ShapeDtypeStruct((n_gy, 4 * levels, bands), jnp.float32),
            ),
            in_specs=[vmem] * 5,
            out_specs=(vmem, vmem),
            scratch_shapes=[
                pltpu.VMEM((xs, levels, rows, cols), jnp.bfloat16),
                pltpu.VMEM((xs, 4 * levels, cols), jnp.bfloat16),
                pltpu.VMEM((ys, levels, bands, rows), jnp.bfloat16),
                pltpu.VMEM((ys, 4 * levels, bands), jnp.float32),
                dma((xs, levels)), dma((xs, levels)), dma((xs,)), dma((xs,)),
                dma((ys, levels)), dma((ys, levels)), dma((ys,)), dma((ys,)),
            ],
            compiler_params=pltpu.CompilerParams(collective_id=0, has_side_effects=True),
        )(field, edge, table, ztable, weights)

        edge_got = edge_got.reshape(n_gy, 4, levels, bands)
        low = lax.dynamic_index_in_dim(edge_got, me_y, 0, keepdims=False)
        high = lax.dynamic_index_in_dim(edge_got, (me_y + 1) % n_gy, 0, keepdims=False)
        low, high = low.transpose(0, 2, 1), high.transpose(0, 2, 1)
        spectra_zone = blend_zone(high[2], high[3], low[0], low[1], EXT_ZONE)

        spectra = jnp.zeros((bands, levels, ny), jnp.float32)
        for shift in range(n_gy):
            full = got[shift].transpose(1, 0, 2).astype(jnp.float32)
            source = (me_y + n_gy - shift) % n_gy
            spectra = lax.dynamic_update_slice(spectra, full, (0, 0, source * rows))
        return spectra, spectra_zone

    return body


ROWS = 128
GROUP = 16


def host_weights(zone_count):
    t = (np.arange(zone_count, dtype=np.float32) + np.float32(1)) / np.float32(zone_count + 1.0)
    two, three, one = np.float32(2), np.float32(3), np.float32(1)
    cube, square = t * t * t, t * t
    return (two * cube - three * square + one, cube - two * square + t,
            three * square - two * cube, cube - square)


def unit_circle(product, length):
    quarter = length / 4.0
    turns = jnp.floor(product * (4.0 / length) + 0.5)
    theta = (product - turns * quarter) * (2.0 * math.pi / length)
    turns = turns - 4.0 * jnp.floor(turns * 0.25)
    z = theta * theta
    sin = theta * (1.0 + z * (-1.0 / 6 + z * (1.0 / 120 + z * (-1.0 / 5040 + z * (1.0 / 362880)))))
    cos = 1.0 + z * (-0.5 + z * (1.0 / 24 + z * (-1.0 / 720 + z * (1.0 / 40320 - z * (1.0 / 3628800)))))
    odd = (turns == 1.0) | (turns == 3.0)
    c, s = jnp.where(odd, sin, cos), jnp.where(odd, cos, sin)
    c = jnp.where((turns == 1.0) | (turns == 2.0), -c, c)
    s = jnp.where(turns >= 2.0, -s, s)
    return c, s


def fused_kernel(n_gx, n_gy, field_ref, out_ref, zone_ref,
                 own, staged, xgot, got, send, tab, ztab, zbuf, pq, cs, acc, esum, esend, egot,
                 ss, ls, xs, xr, zs, zr, fs, fr, far, *, depth, lags):
    levels, rows, cols = field_ref.shape
    bands = got.shape[2]
    nblk, share = rows // ROWS, levels // n_gx
    half = n_gy // 2 * n_gx * bands
    nx = n_gx * cols
    length = nx + EXT_ZONE
    me_x, me_y = lax.axis_index("gx"), lax.axis_index("gy")
    chunks = share * nblk
    blocks = [(k, x) for k in range(n_gy - 1) for x in range(n_gx)]
    blocks += [(n_gy - 1, x) for x in range(1, n_gx)] + [(n_gy - 1, 0)]

    def peer_x(shift):
        return {"gx": lax.rem(me_x + n_gx - shift, n_gx)}

    def peer_y(shift):
        return {"gy": lax.rem(me_y + shift, n_gy)}

    def turn(k):
        up, down = n_gy - 1 - k, k
        if k == n_gy - 1:
            return 0
        up = jnp.where(up > me_y, up, up - 1)
        down = jnp.where(down < me_y, down, down + 1)
        return lax.rem(jnp.where(2 * me_y < n_gy, up, down) - me_y + n_gy, n_gy)

    above, below = me_y < n_gy - 1, me_y > 0

    def tell(semaphore, up):
        pl.semaphore_signal(semaphore, inc=1, device_id={"gy": me_y + (1 if up else -1)},
                            device_id_type=MESH)

    barrier = pltpu.get_barrier_semaphore()
    for shift in range(1, n_gx):
        pl.semaphore_signal(barrier, inc=1, device_id=peer_x(shift), device_id_type=MESH)
    pl.when(above)(lambda: tell(barrier, True))
    pl.when(below)(lambda: tell(barrier, False))

    def vouch():
        pl.when(above & below)(lambda: tell(far.at[0], False))
        pl.when(above & below)(lambda: tell(far.at[1], True))

    def hear():
        for hop in range(n_gy - 2):
            @pl.when(me_y + hop < n_gy - 2)
            def _():
                pl.semaphore_wait(far.at[0], 1)
                pl.when(below)(lambda: tell(far.at[0], False))

            @pl.when(me_y - hop > 1)
            def _():
                pl.semaphore_wait(far.at[1], 1)
                pl.when(above)(lambda: tell(far.at[1], True))

        for shift in range(1, n_gx):
            pl.semaphore_signal(far.at[2], inc=1, device_id=peer_x(shift), device_id_type=MESH)
        pl.semaphore_wait(far.at[2], n_gx - 1)

    def place(i, owner):
        ahead = jnp.where(owner == n_gy - 1, nblk - 1, 0)
        return lax.rem(i // share + ahead, nblk), lax.rem(i, share)

    def lines(blk):
        return pl.ds(pl.multiple_of(blk * ROWS, ROWS), ROWS)

    def load(turn_at):
        blk, _ = place(turn_at * share, me_y)
        at = lines(blk)
        return pltpu.make_async_copy(
            field_ref.at[pl.ds(me_x * share, share), at], own.at[:, at], ls.at[turn_at])

    def stage(shift):
        blk, _ = place(0, me_y)
        return pltpu.make_async_copy(
            field_ref.at[peer_x(shift)["gx"] * share, lines(blk)], staged.at[shift - 1], ss.at[shift - 1])

    def rows_x(shift, i, source=None):
        blk, level = place(i, me_y)
        at = lines(blk)
        peer = peer_x(shift)
        if source is None:
            source = field_ref.at[peer["gx"] * share + level, at]
        return pltpu.make_async_remote_copy(
            src_ref=source, dst_ref=xgot.at[shift - 1, level, at],
            send_sem=xs.at[shift - 1], recv_sem=xr.at[i], device_id=peer, device_id_type=MESH)

    def rows_in(i):
        blk, level = place(i, me_y)
        ref = xgot.at[:, level, lines(blk)]
        return pltpu.make_async_remote_copy(
            src_ref=ref, dst_ref=ref, send_sem=xs.at[0], recv_sem=xr.at[i],
            device_id=peer_x(1), device_id_type=MESH)

    def owner_of(b):
        k, x = blocks[b]
        return {"gy": lax.rem(me_y + turn(k), n_gy), "gx": lax.rem(me_x + x, n_gx)}

    def spec(b, i):
        return pltpu.make_async_remote_copy(
            src_ref=send.at[b, i], dst_ref=got.at[me_y * n_gx + me_x, i],
            send_sem=zs, recv_sem=zr.at[i], device_id=owner_of(b), device_id_type=MESH)

    def specs_in(i):
        return pltpu.make_async_remote_copy(
            src_ref=send.at[:, 0], dst_ref=got.at[pl.ds(0, len(blocks) - 1), 0],
            send_sem=zs, recv_sem=zr.at[i], device_id=peer_y(1), device_id_type=MESH)

    def edge(side, b):
        return pltpu.make_async_remote_copy(
            src_ref=esend.at[b], dst_ref=egot.at[side, me_x], send_sem=fs, recv_sem=fr.at[side, me_x],
            device_id=owner_of(b), device_id_type=MESH)

    def edge_in(side, x):
        return pltpu.make_async_remote_copy(
            src_ref=esend.at[0], dst_ref=egot.at[side, x], send_sem=fs, recv_sem=fr.at[side, x],
            device_id=peer_y(1), device_id_type=MESH)

    def all_sent(ref, semaphore):
        pltpu.make_async_remote_copy(
            src_ref=ref, dst_ref=ref, send_sem=semaphore, recv_sem=fr.at[0, 0],
            device_id=peer_y(1), device_id_type=MESH).wait_send()

    for shift in range(1, n_gx):
        stage(shift).start()
    for turn_at in range(nblk):
        load(turn_at).start()

    pl.semaphore_wait(barrier, n_gx - 1 + above.astype(jnp.int32) + below.astype(jnp.int32))

    def send_ahead():
        for shift in range(1, n_gx):
            stage(shift).wait()
            rows_x(shift, 0, staged.at[shift - 1]).start()

        @pl.loop(1, depth)
        def _(i):
            for shift in range(1, n_gx):
                rows_x(shift, i).start()

    leads = lax.axis_index("lev") != 0
    lag = jnp.where(leads, *lags)
    pl.when(leads)(send_ahead)
    vouch()

    norm = 1.0 / math.sqrt(length)
    ngroup = half // GROUP
    lane = lax.broadcasted_iota(jnp.int32, (1, LANES), 1)

    def build(part):
        row0 = part * half
        g = lax.broadcasted_iota(jnp.int32, (ngroup, 1), 0) * GROUP + row0
        block = g // bands
        origin = jnp.zeros((ngroup, 1), jnp.int32)
        for b in range(row0 // bands, (row0 + half) // bands):
            to = owner_of(b)
            origin = jnp.where(block == b, (to["gy"] * n_gx + to["gx"]) * bands, origin)
        first = origin + (g - block * bands)
        is_cos = first < nx // 2
        number = jnp.where(is_cos, first, first - (nx // 2 - 1)).astype(jnp.float32)
        step = lax.broadcasted_iota(jnp.int32, (GROUP, 1), 0).astype(jnp.float32)

        def factors(column, width):
            c, s = unit_circle(number * column, length)
            pq[0, :, :width], pq[1, :, :width] = jnp.where(is_cos, c, -s), jnp.where(is_cos, s, c)
            c, s = unit_circle(step * column, length)
            cs[0, :, :width], cs[1, :, :width] = c * norm, s * norm

        def expand(write, width):
            @pl.loop(0, ngroup // 8)
            def _(k):
                at = pl.ds(pl.multiple_of(k * 8, 8), 8)
                for r in range(8):
                    p, q = pq[0, at, :width][r:r + 1], pq[1, at, :width][r:r + 1]
                    write(pl.ds(pl.multiple_of(row0 + (k * 8 + r) * GROUP, GROUP), GROUP),
                          p * cs[0, :, :width] - q * cs[1, :, :width])

        for at in range(n_gx):
            base = (lax.rem(me_x + at, n_gx) * cols).astype(jnp.float32)
            factors(lax.broadcasted_iota(jnp.int32, (1, cols), 1).astype(jnp.float32) + base, cols)

            def write(to, value, at=at):
                tab[at, to, :] = value.astype(jnp.bfloat16)

            expand(write, cols)
            if part == 0 and at == 0:
                pl.when(jnp.logical_not(leads))(send_ahead)
        factors(lane.astype(jnp.float32) + float(nx), LANES)

        def write_zone(to, value):
            ztab[to, :] = jnp.where(lane < EXT_ZONE, value, 0.0).astype(jnp.bfloat16)

        expand(write_zone, LANES)

    t = jnp.minimum(lane + 1, EXT_ZONE).astype(jnp.float32) / (EXT_ZONE + 1.0)
    cube, square = t * t * t, t * t
    weight_a = 2.0 * cube - 3.0 * square + 1.0
    weight_b = cube - 2.0 * square + t
    weight_c = -2.0 * cube + 3.0 * square
    weight_d = cube - square
    tangent = EXT_ZONE + 1.0
    tail = cols - LANES

    def zone_of(parts):
        first = second = last = before = 0.0
        for at, part in enumerate(parts):
            owner = lax.rem(me_x + at, n_gx)
            is_first = jnp.where(owner == 0, 1.0, 0.0)
            is_last = jnp.where(owner == n_gx - 1, 1.0, 0.0)
            head = part[:, :LANES].astype(jnp.float32)
            rear = part[:, tail:].astype(jnp.float32)
            first += is_first * head[:, 0:1]
            second += is_first * head[:, 1:2]
            before += is_last * rear[:, LANES - 2:LANES - 1]
            last += is_last * rear[:, LANES - 1:LANES]
        zone = (last * weight_a + (tangent * (last - before)) * weight_b
                + first * weight_c + (tangent * (second - first)) * weight_d)
        return zone.astype(jnp.bfloat16)

    def dot(a, b):
        return lax.dot_general(a, b, NT, preferred_element_type=jnp.float32)

    def arrive(i):
        specs_in(i).wait_recv()
        for source in range(n_gy * n_gx):
            blk, level = place(i, source // n_gx)
            level += source % n_gx * share
            out_ref[source // n_gx * nblk + blk, pl.ds(level, bands, stride=levels), :] = (
                got[source, i].astype(jnp.float32))

    def own_part(i, part):
        blk, level = place(i, me_y)
        at = pl.ds(part * half, half)
        acc[at, :] = dot(tab[0, at, :], own[level, lines(blk), :])

    def blend(i):
        blk, level = place(i, me_y)
        at = lines(blk)
        zbuf[...] = zone_of([own[level, at, :]] + [xgot[x, level, at, :] for x in range(n_gx - 1)])

    def finish(i, lo, hi):
        blk, level = place(i, me_y)
        at = pl.ds(lo * bands, (hi - lo) * bands)
        total = acc[at, :] + dot(ztab[at, :], zbuf[...])
        for x in range(1, n_gx):
            total += dot(tab[x, at, :], xgot[x - 1, level, lines(blk), :])
        for b in range(lo, hi):
            piece = total[(b - lo) * bands:(b - lo + 1) * bands].astype(jnp.bfloat16)
            if b == len(blocks) - 1:
                got[me_y * n_gx + me_x, i] = piece
            else:
                send[b, i] = piece
                spec(b, i).start()

    def far_pieces(i):
        for lo in range(0, half // bands, n_gx):
            finish(i, lo, lo + n_gx)

    def near_pieces(i):
        finish(i, half // bands, len(blocks))

    def edges():
        top = me_y == 0
        row0 = pl.multiple_of(jnp.where(top, 0, rows - 16), 16)
        parts = [own[:, pl.ds(row0, 16), :].reshape(share * 16, cols)]
        parts += [xgot[x, :, pl.ds(row0, 16), :].reshape(share * 16, cols) for x in range(n_gx - 1)]
        total = dot(zone_of(parts), ztab[...])
        for x, part in enumerate(parts):
            total += dot(part, tab[x])
        esum[...] = total
        for pair in range(2):
            for level in range(share):
                upper = esum[level * 16 + pair:level * 16 + pair + 1, :]
                lower = esum[level * 16 + 14 + pair:level * 16 + 15 + pair, :]
                line = jnp.where(top, upper, lower)
                row = pair * share + level
                for b in range(len(blocks)):
                    esend[b, row:row + 1, :] = line[:, b * bands:(b + 1) * bands]
        for side, owner in ((0, 0), (1, n_gy - 1)):
            @pl.when(me_y == owner)
            def _(side=side):
                egot[side, me_x] = esend[len(blocks) - 1]
                for b in range(len(blocks) - 1):
                    edge(side, b).start()

    seam = (me_y == 0) | (me_y == n_gy - 1)

    def rows_ready(i):
        rows_in(i).wait_recv()

        @pl.when(i + depth < chunks)
        def _():
            for shift in range(1, n_gx):
                rows_x(shift, i + depth).start()

        blend(i)

    build(0)
    load(0).wait()
    own_part(0, 0)
    hear()
    rows_ready(0)
    far_pieces(0)
    build(1)
    own_part(0, 1)
    near_pieces(0)

    @pl.loop(1, chunks)
    def _(i):
        for turn_at in range(1, nblk):
            @pl.when(i == turn_at * share)
            def _():
                load(turn_at).wait()

        own_part(i, 0)
        own_part(i, 1)
        rows_ready(i)
        far_pieces(i)
        near_pieces(i)

        @pl.when(seam & (i == share - 1))
        def _():
            edges()

        @pl.when(i >= lag)
        def _():
            arrive(i - lag)

    for side, owner in ((0, 0), (1, n_gy - 1)):
        for x in range(n_gx):
            @pl.when((me_y != owner) | (me_x != x))
            def _(side=side, x=x):
                edge_in(side, x).wait_recv()

    pl.when(seam)(lambda: all_sent(esend.at[pl.ds(0, len(blocks) - 1)], fs))
    wa, wb, wc, wd = host_weights(EXT_ZONE)
    for x in range(n_gx):
        first, second = egot[0, x, :share, :], egot[0, x, share:, :]
        before, last = egot[1, x, :share, :], egot[1, x, share:, :]
        slope_start, slope_end = tangent * (last - before), tangent * (second - first)
        for j in range(EXT_ZONE):
            zone_ref[j, x * share:(x + 1) * share, :] = (
                last * float(wa[j]) + slope_start * float(wb[j])
                + first * float(wc[j]) + slope_end * float(wd[j]))

    for shift in range(1, n_gx):
        all_sent(field_ref.at[pl.ds(0, share)], xs.at[shift - 1])

    @pl.loop(chunks - lag, chunks)
    def _(i):
        arrive(i)

    all_sent(send, zs)


def make_fused_body(mesh):
    n_gx, n_gy = mesh.shape["gx"], mesh.shape["gy"]

    def body(field):
        levels, rows, cols = field.shape
        bands = cols // n_gy
        nblk, ny, size = rows // ROWS, rows * n_gy, n_gy * n_gx * bands
        share, xs, peers = levels // n_gx, n_gx - 1, n_gy * n_gx - 1
        chunks = share * nblk
        vmem, dma = pl.BlockSpec(memory_space=pltpu.VMEM), pltpu.SemaphoreType.DMA
        bf16, f32 = jnp.bfloat16, jnp.float32
        spectra, zone = pl.pallas_call(
            functools.partial(fused_kernel, n_gx, n_gy, depth=DEPTH, lags=(LAG_LEAD, LAG)),
            out_shape=(
                jax.ShapeDtypeStruct((n_gy * nblk, bands * levels, ROWS), f32),
                jax.ShapeDtypeStruct((EXT_ZONE, levels, bands), f32),
            ),
            in_specs=[pl.BlockSpec(memory_space=pltpu.HBM)],
            out_specs=(vmem, vmem),
            scratch_shapes=[
                pltpu.VMEM((share, rows, cols), bf16),
                pltpu.VMEM((xs, ROWS, cols), bf16),
                pltpu.VMEM((xs, share, rows, cols), bf16),
                pltpu.VMEM((peers + 1, chunks, bands, ROWS), bf16),
                pltpu.VMEM((peers, chunks, bands, ROWS), bf16),
                pltpu.VMEM((n_gx, size, cols), bf16),
                pltpu.VMEM((size, LANES), bf16),
                pltpu.VMEM((ROWS, LANES), bf16),
                pltpu.VMEM((2, size // 2 // GROUP, cols), f32),
                pltpu.VMEM((2, GROUP, cols), f32),
                pltpu.VMEM((size, ROWS), f32),
                pltpu.VMEM((share * 16, size), f32),
                pltpu.VMEM((peers + 1, 2 * share, bands), f32),
                pltpu.VMEM((2, n_gx, 2 * share, bands), f32),
                dma((xs,)), dma((nblk,)), dma((xs,)), dma((chunks,)), dma, dma((chunks,)),
                dma, dma((2, n_gx)), pltpu.SemaphoreType.REGULAR((3,)),
            ],
            compiler_params=pltpu.CompilerParams(
                collective_id=0, has_side_effects=True, vmem_limit_bytes=VMEM_LIMIT),
        )(pltpu.with_memory_space_constraint(field, pltpu.HBM))
        spectra, zone = pl.pallas_call(
            store_kernel,
            out_shape=(
                jax.ShapeDtypeStruct((bands * levels, ny), f32),
                jax.ShapeDtypeStruct(zone.shape, f32),
            ),
            in_specs=[vmem, vmem],
            out_specs=(pl.BlockSpec(memory_space=pl.ANY),) * 2,
            scratch_shapes=[dma((n_gy * nblk + 1,))],
            compiler_params=pltpu.CompilerParams(vmem_limit_bytes=VMEM_LIMIT_STORE),
        )(spectra, zone)
        return spectra.reshape(bands, levels, ny), zone.transpose(2, 1, 0)

    return body


def store_kernel(tile_ref, zone_ref, out_ref, zone_out_ref, sem):
    count = tile_ref.shape[0]
    copies = [
        pltpu.make_async_copy(tile_ref.at[b], out_ref.at[:, pl.ds(b * ROWS, ROWS)], sem.at[b])
        for b in range(count)
    ]
    copies.append(pltpu.make_async_copy(zone_ref, zone_out_ref, sem.at[count]))
    for copy in copies:
        copy.start()
    for copy in copies:
        copy.wait()


VMEM_LIMIT_STORE = 16 * 2**20
DEPTH = 3
LAG_LEAD = 1
LAG = 4
VMEM_LIMIT = 36 * 2**20


def fits(mesh, shape):
    n_gx, n_gy = mesh.shape["gx"], mesh.shape["gy"]
    levels = shape[0] // (mesh.shape["member"] * mesh.shape["lev"])
    rows, cols = shape[1] // n_gy, shape[2] // n_gx
    bands = cols // n_gy
    return (n_gx > 1 and n_gy > 1 and n_gy % 2 == 0 and rows % ROWS == 0 and cols % LANES == 0
            and bands % GROUP == 0 and n_gy * n_gx * bands % (16 * GROUP) == 0
            and (cols * n_gx // 2) % bands == 0 and levels % 8 == 0 and levels % (2 * n_gx) == 0
            and levels // n_gx * rows // ROWS > max(DEPTH, LAG))


def solution(mesh):
    def program(field):
        body = make_fused_body(mesh) if fits(mesh, field.shape) else make_plain_body(mesh)
        return jax.shard_map(
            body,
            mesh=mesh,
            in_specs=(P(("member", "lev"), "gy", "gx"),),
            out_specs=(
                P(("gy", "gx"), ("member", "lev"), None),
                P(("gy", "gx"), ("member", "lev"), None),
            ),
            check_vma=False,
        )(field)

    return program
```
